32 devices in a mesh: grp: 4 (over z), seq: 8 (over y, x, core).
Axes of the slice: x: 2, y: 2, z: 4, core: 2. Of those that a mesh axis runs over, the one named last changes fastest.
Arguments:
- hidden_in: bfloat16 [24, 4096], P(None, ('grp', 'seq')), may hold values from -6 to 6
- norm_gain: float32 [4096], replicated, may hold values from 0.5 to 1.5
- w_ssm_in: bfloat16 [4096, 8192], P(None, ('grp', 'seq')), may hold values from -0.09375 to 0.09375
- w_ssm_gate: bfloat16 [4096, 8192], P(None, ('grp', 'seq')), may hold values from -0.09375 to 0.09375
- conv_weight: float32 [4, 8192], P(None, ('grp', 'seq')), may hold values from -3 to 3
- conv_bias: float32 [8192], P(('grp', 'seq')), may hold values from -0.5 to 0.5
- conv_state: bfloat16 [24, 3, 8192], P(None, None, ('grp', 'seq')), may hold values from -6 to 6
- w_state_proj: bfloat16 [8192, 288], P(('grp', 'seq')), may hold values from -0.0625 to 0.0625
- w_step: bfloat16 [256, 8192], P(None, ('grp', 'seq')), may hold values from -0.375 to 0.375
- step_bias: float32 [8192], P(('grp', 'seq')), may hold values from -4 to -1
- log_decay: float32 [16, 8192], P(None, ('grp', 'seq')), may hold values from 0 to 2.7
- skip_gain: float32 [8192], P(('grp', 'seq')), may hold values from 0.5 to 1.5
- ssm_state: float32 [24, 16, 8192], P(None, None, ('grp', 'seq')), may hold values from -6 to 6
- w_ssm_out: bfloat16 [8192, 4096], P(('grp', 'seq')), may hold values from -0.125 to 0.125
- w_query: bfloat16 [4096, 2048], P(None, 'grp'), may hold values from -6 to 6
- key_projection: bfloat16 [4096, 1024], P(None, 'grp'), may hold values from -0.09375 to 0.09375
- value_projection: bfloat16 [4096, 1024], P(None, 'grp'), may hold values from -0.09375 to 0.09375
- w_attn_out: bfloat16 [2048, 4096], P('grp', 'seq'), may hold values from -0.125 to 0.125
- w_mlp_gate: bfloat16 [4096, 14336], P(None, ('grp', 'seq')), may hold values from -0.09375 to 0.09375
- w_mlp_up: bfloat16 [4096, 14336], P(None, ('grp', 'seq')), may hold values from -0.09375 to 0.09375
- w_mlp_down: bfloat16 [14336, 4096], P(('grp', 'seq')), may hold values from -0.09375 to 0.09375
- cached_inputs: bfloat16 [24, 512, 4096], P('seq'), may hold values from -6 to 6
- window_lengths: int32 [24], replicated, may hold values from 1 to 512, as said below
Outputs:
- hidden_out: bfloat16 [24, 4096], P(None, ('grp', 'seq'))
- state_out: float32 [24, 16, 8192], P(None, None, ('grp', 'seq'))
The draws below stay inside these ranges and needn't reach their ends.
Inputs may be any that keep to these rules, and one draw needn't show every extreme that they name: `window_lengths`: every sequence has at least one valid cached position, and some sequence fills the whole window of 512.
All inputs are finite; a program needn't handle non-finite values.
Results may differ from the reference program's by a relative error of at most 0.012.
The reference program's roundings to bfloat16 on the way count: a program that leaves them out, or rounds other values in their place, can miss the bound.
Values may be sent and summed in bfloat16 or wider, within the bound.
A program may use at most 128 MiB of HBM per device.

```python
import jax
import jax.numpy as jnp
from jax import lax

MODEL_DIM = 4096
E = 8192
NS = 16
KC = 4
DTR = 256
QUERY_HEADS = 16
KEY_VALUE_HEADS = 8
HEAD_SIZE = 128
FF = 14336
WINDOW_SPAN = 512
BATCH_SEQUENCES = 24


def draw_window_lengths(key, part):
    drawn_lengths = jax.random.randint(jax.random.fold_in(key, 7), (BATCH_SEQUENCES,), 1, WINDOW_SPAN + 1, dtype=jnp.int32)
    chosen = jax.random.randint(jax.random.fold_in(key, 11), (), 0, BATCH_SEQUENCES, dtype=jnp.int32)
    return jnp.where(jnp.arange(BATCH_SEQUENCES, dtype=jnp.int32) == chosen, WINDOW_SPAN, drawn_lengths).astype(jnp.int32)


def draw_w_query(key, part):
    columns = QUERY_HEADS * HEAD_SIZE
    chosen_heads = jax.random.permutation(jax.random.fold_in(key, 3), QUERY_HEADS)
    entries = jax.random.normal(jax.random.fold_in(key, 5), (MODEL_DIM, columns), jnp.float32)
    levels = jnp.array([24.0, 48.0, 96.0], jnp.float32)
    head_scale = jnp.ones((QUERY_HEADS,), jnp.float32).at[chosen_heads[:3]].set(levels)
    column_scale = jnp.repeat(head_scale, HEAD_SIZE)
    scaled = entries * column_scale[None, :] * float(MODEL_DIM) ** (-0.5)
    return jnp.clip(scaled, -6.0, 6.0).astype(jnp.bfloat16)


def spiked(values, key, source, target, blocks, factor):
    def block_of(axis_at):
        return (jnp.arange(values.shape[axis_at]) // (values.shape[axis_at] // blocks)).reshape((-1,) + (1,) * (values.ndim - 1 - axis_at))

    one_side = jax.random.permutation(key, blocks)[block_of(target)]
    far = (block_of(target) + blocks // 2) % blocks
    return jnp.where((block_of(source) == one_side) | (block_of(source) == far), factor * values, values)


def level_of(stream_key, dims, shards, least, high):
    loudness, own = 1.0, jax.random.fold_in(stream_key, 6)
    for dim, shards_of in shards:
        draws = jnp.exp(jax.random.uniform(jax.random.fold_in(own, dim), (shards_of,), jnp.float32, least / len(shards), high / len(shards)))
        loudness = loudness * jnp.repeat(draws, dims[dim] // shards_of).reshape([-1 if axis == dim else 1 for axis in range(len(dims))])
    return loudness


def bell_draw(stream_key, dims, scale, reach, pieces=(), held_as=jnp.bfloat16):
    level = level_of(stream_key, dims, pieces, -0.22, 0.18) if pieces else 1.0
    values = jax.random.normal(stream_key, dims, jnp.float32) * scale * level
    return jnp.minimum(jnp.maximum(values, -reach), reach).astype(held_as)


def noise_with(rng, extent, deviation, limit, shards, heavy, kind=jnp.bfloat16):
    drawn = deviation * jax.random.normal(rng, extent, jnp.float32)
    if shards:
        drawn = drawn * level_of(rng, extent, shards, -0.22, 0.18)
    return jnp.clip(spiked(drawn, jax.random.fold_in(rng, 3), *heavy), -limit, limit).astype(kind)


def setup_inputs(seed: int = 0) -> dict:
    key_list = jax.random.split(jax.random.key(seed), 24)
    return {
        "hidden_in": bell_draw(key_list[0], (BATCH_SEQUENCES, MODEL_DIM), 1.0, 6.0, ((1, 32),)),
        "norm_gain": jnp.clip(1.0 + 0.1 * jax.random.normal(key_list[1], (MODEL_DIM,), jnp.float32), 0.5, 1.5),
        "w_ssm_in": bell_draw(key_list[2], (MODEL_DIM, E), MODEL_DIM ** -0.5, 0.09375, ((1, 32),)),
        "w_ssm_gate": bell_draw(key_list[3], (MODEL_DIM, E), MODEL_DIM ** -0.5, 0.09375, ((1, 32),)),
        "conv_weight": bell_draw(key_list[4], (KC, E), KC ** -0.5, 3.0, ((1, 32),), jnp.float32),
        "conv_bias": jnp.clip(jax.random.uniform(key_list[5], (E,), jnp.float32, -0.5, 0.5) * level_of(key_list[5], (E,), ((0, 32),), -0.4, 0.0), -0.5, 0.5),
        "conv_state": bell_draw(key_list[6], (BATCH_SEQUENCES, KC - 1, E), 1.0, 6.0, ((2, 32),)),
        "w_state_proj": bell_draw(key_list[7], (E, DTR + 2 * NS), E ** -0.5, 0.0625, ((0, 32),)),
        "w_step": bell_draw(key_list[8], (DTR, E), DTR ** -0.5, 0.375, ((1, 32),)),
        "step_bias": jnp.clip(-4.0 + 3.0 * jax.random.uniform(key_list[9], (E,), jnp.float32) ** level_of(key_list[9], (E,), ((0, 32),), -0.2, 0.2), -4.0, -1.0),
        "log_decay": jnp.clip(2.7 * jax.random.uniform(key_list[10], (NS, E), jnp.float32) ** level_of(key_list[10], (NS, E), ((1, 32),), -0.2, 0.2), 0.0, 2.7),
        "skip_gain": jnp.clip(0.5 + 1.0 * jax.random.uniform(key_list[11], (E,), jnp.float32) ** level_of(key_list[11], (E,), ((0, 32),), -0.2, 0.2), 0.5, 1.5),
        "ssm_state": bell_draw(key_list[12], (BATCH_SEQUENCES, NS, E), 1.0, 6.0, ((2, 32),), jnp.float32),
        "w_ssm_out": noise_with(key_list[13], (E, MODEL_DIM), E ** -0.5, 0.125, ((0, 32),), (0, 1, 32, 2.75)),
        "w_query": draw_w_query(jax.random.fold_in(key_list[23], 71), 0),
        "key_projection": bell_draw(key_list[15], (MODEL_DIM, KEY_VALUE_HEADS * HEAD_SIZE), MODEL_DIM ** -0.5, 0.09375, ((1, 4),)),
        "value_projection": bell_draw(key_list[16], (MODEL_DIM, KEY_VALUE_HEADS * HEAD_SIZE), MODEL_DIM ** -0.5, 0.09375, ((1, 4),)),
        "w_attn_out": bell_draw(key_list[17], (QUERY_HEADS * HEAD_SIZE, MODEL_DIM), (QUERY_HEADS * HEAD_SIZE) ** -0.5, 0.125, ((0, 4), (1, 8))),
        "w_mlp_gate": bell_draw(key_list[18], (MODEL_DIM, FF), MODEL_DIM ** -0.5, 0.09375, ((1, 32),)),
        "w_mlp_up": bell_draw(key_list[19], (MODEL_DIM, FF), MODEL_DIM ** -0.5, 0.09375, ((1, 32),)),
        "w_mlp_down": noise_with(key_list[20], (FF, MODEL_DIM), FF ** -0.5, 0.09375, ((0, 32),), (0, 1, 32, 2.75)),
        "cached_inputs": bell_draw(key_list[21], (BATCH_SEQUENCES, WINDOW_SPAN, MODEL_DIM), 1.0, 6.0, ((0, 8),)),
        "window_lengths": draw_window_lengths(jax.random.fold_in(key_list[23], 71), 0),
    }


epsilon = 1e-05
rope_base = 10000.0

def apply_rotary(head_values, positions):
    half_dim = head_values.shape[-1] // 2
    frequency = rope_base ** (-(jnp.arange(half_dim, dtype=jnp.float32) * 2.0) / head_values.shape[-1])
    angles = positions[..., None, None] * frequency
    cosine = jnp.cos(angles)
    sine_part = jnp.sin(angles)
    front_half = head_values[..., :half_dim]
    back_half = head_values[..., half_dim:]
    return jnp.concatenate([front_half * cosine - back_half * sine_part, back_half * cosine + front_half * sine_part], axis=-1)

def reference(hidden_in, norm_gain, w_ssm_in, w_ssm_gate, conv_weight, conv_bias, conv_state, w_state_proj, w_step, step_bias, log_decay, skip_gain, ssm_state, w_ssm_out, w_query, key_projection, value_projection, w_attn_out, w_mlp_gate, w_mlp_up, w_mlp_down, cached_inputs, window_lengths):
    hidden_f = hidden_in.astype(jnp.float32)
    row_scale = lax.rsqrt(lax.optimization_barrier(jnp.mean(hidden_f * hidden_f, axis=1, keepdims=True)) + epsilon)
    normed_input = (hidden_f * row_scale * norm_gain).astype(jnp.bfloat16)
    ssm_input = jnp.dot(normed_input, w_ssm_in, preferred_element_type=jnp.float32).astype(jnp.bfloat16)
    gate_input = jnp.dot(normed_input, w_ssm_gate, preferred_element_type=jnp.float32)
    past_inputs = conv_state.astype(jnp.float32)
    conv_sum = conv_bias + lax.optimization_barrier(jnp.sum(past_inputs * conv_weight[:-1][None], axis=1)) + conv_weight[-1] * lax.optimization_barrier(ssm_input).astype(jnp.float32)
    conv_out = jax.nn.silu(conv_sum)
    low_rank = jnp.dot(conv_out.astype(jnp.bfloat16), w_state_proj, preferred_element_type=jnp.float32)
    step_low = low_rank[:, :DTR].astype(jnp.bfloat16)
    input_map = low_rank[:, DTR:DTR + NS]
    output_map = low_rank[:, DTR + NS:]
    step_size = jax.nn.softplus(jnp.dot(step_low, w_step, preferred_element_type=jnp.float32) + step_bias)
    decay_rate = jnp.exp(log_decay)
    state_out = jnp.exp(-step_size[:, None, :] * decay_rate[None]) * ssm_state + step_size[:, None, :] * input_map[:, :, None] * conv_out[:, None, :]
    ssm_mixed = lax.optimization_barrier(jnp.sum(state_out * output_map[:, :, None], axis=1)) + skip_gain * conv_out
    ssm_gated = (ssm_mixed * jax.nn.silu(gate_input)).astype(jnp.bfloat16)
    ssm_term = jnp.dot(ssm_gated, w_ssm_out, preferred_element_type=jnp.float32)
    gate_act = jnp.dot(normed_input, w_mlp_gate, preferred_element_type=jnp.float32)
    up_act = jnp.dot(normed_input, w_mlp_up, preferred_element_type=jnp.float32)
    mlp_hidden = (jax.nn.silu(gate_act) * up_act).astype(jnp.bfloat16)
    mlp_term = jnp.dot(mlp_hidden, w_mlp_down, preferred_element_type=jnp.float32)
    fresh_position = window_lengths.astype(jnp.float32)
    query = apply_rotary(jnp.dot(normed_input, w_query, preferred_element_type=jnp.float32).reshape(BATCH_SEQUENCES, QUERY_HEADS, HEAD_SIZE), fresh_position).astype(jnp.bfloat16)
    fresh_key = apply_rotary(jnp.dot(normed_input, key_projection, preferred_element_type=jnp.float32).reshape(BATCH_SEQUENCES, KEY_VALUE_HEADS, HEAD_SIZE), fresh_position).astype(jnp.bfloat16)
    fresh_value = jnp.dot(normed_input, value_projection, preferred_element_type=jnp.float32).astype(jnp.bfloat16).reshape(BATCH_SEQUENCES, KEY_VALUE_HEADS, HEAD_SIZE)
    heads_per_group = QUERY_HEADS // KEY_VALUE_HEADS
    attention_scale = HEAD_SIZE ** (-0.5)

    def one_row(row_args):
        window_row_inputs, query_for_row, row_key, row_value, row_length = row_args
        slot_ids = jnp.arange(WINDOW_SPAN, dtype=jnp.int32)
        window_key_rows = jnp.dot(window_row_inputs, key_projection, preferred_element_type=jnp.float32).reshape(WINDOW_SPAN, KEY_VALUE_HEADS, HEAD_SIZE)
        window_key_rows = apply_rotary(window_key_rows, slot_ids.astype(jnp.float32)).astype(jnp.bfloat16)
        window_value_rows = jnp.dot(window_row_inputs, value_projection, preferred_element_type=jnp.float32).astype(jnp.bfloat16).reshape(WINDOW_SPAN, KEY_VALUE_HEADS, HEAD_SIZE)
        grouped_query = query_for_row.astype(jnp.float32).reshape(KEY_VALUE_HEADS, heads_per_group, HEAD_SIZE)
        scores = jnp.einsum('kgd,wkd->kgw', grouped_query, window_key_rows.astype(jnp.float32)) * attention_scale
        fresh_score = jnp.einsum('kgd,kd->kg', grouped_query, row_key.astype(jnp.float32)) * attention_scale
        is_valid = slot_ids < row_length
        scores = jnp.where(is_valid[None, None, :], scores, -1e+30)
        row_max = jnp.maximum(lax.optimization_barrier(jnp.max(scores, axis=-1)), fresh_score)
        weights = jnp.where(is_valid[None, None, :], jnp.exp(scores - row_max[..., None]), 0.0)
        weight_new = jnp.exp(fresh_score - row_max)
        row_total = lax.optimization_barrier(jnp.sum(weights, axis=-1)) + weight_new
        weighted = jnp.einsum('kgw,wkd->kgd', weights, window_value_rows.astype(jnp.float32)) + weight_new[..., None] * row_value.astype(jnp.float32)[:, None, :]
        return (weighted / row_total[..., None]).reshape(QUERY_HEADS * HEAD_SIZE).astype(jnp.bfloat16)
    attended = lax.map(one_row, (cached_inputs, query, fresh_key, fresh_value, window_lengths))
    attn_term = jnp.dot(attended, w_attn_out, preferred_element_type=jnp.float32)
    hidden_out = (hidden_f + (ssm_term + mlp_term + attn_term)).astype(jnp.bfloat16)
    return (hidden_out, state_out)
```

```python
import functools

import jax
import jax.numpy as jnp
import numpy as np
from jax import lax
from jax.experimental import pallas as pl
from jax.experimental.pallas import tpu as pltpu
from jax.sharding import PartitionSpec as P

HEAD_SIZE = 128
MESH = pl.DeviceIdType.MESH
VMEM_LIMIT = 66_000_000

epsilon = 1e-05
rope_base = 10000.0

bf16 = jnp.bfloat16
f32 = jnp.float32


def dot_nn(a, b):
    return jnp.dot(a, b, preferred_element_type=f32)


def dot_nt(a, b):
    return lax.dot_general(a, b, (((1,), (1,)), ((), ())), preferred_element_type=f32)


def silu(v):
    return v / (1.0 + jnp.exp(-v))


def turned(values, cosine, sine):
    return (values * cosine + pltpu.roll(values, HEAD_SIZE // 2, 1) * sine).astype(bf16)


OPERANDS = (
    "hidden",
    "gain",
    "w_in",
    "w_gate",
    "conv_w",
    "conv_b",
    "conv_s",
    "w_state",
    "w_step",
    "step_b",
    "decay",
    "skip",
    "state",
    "w_out",
    "w_query",
    "w_key",
    "w_value",
    "w_attn",
    "m_gate",
    "m_up",
    "m_down",
    "cached",
    "lengths",
    "cosine",
    "sine",
)


def step_kernel(groups, seq_size, rank, tile, *refs):
    count = len(OPERANDS)
    hbm = dict(zip(OPERANDS, refs[:count]))
    out_ref, state_out_ref = refs[count : count + 2]
    held = dict(zip(OPERANDS, refs[count + 2 : 2 * count + 2]))
    (
        gathered,
        normed_ref,
        keys,
        values,
        query_rows,
        key_rows,
        value_rows,
        part_src,
        part_land,
        plane_src,
        plane_land,
        low_ref,
        step_ref,
        conv_ref,
        mix_ref,
        gate_ref,
        att_src,
        att_land,
        term,
        outgoing,
        landed,
        in_sem,
        x_sem,
        out_sem,
        gather_send,
        gather_recv,
        part_send,
        part_recv,
        plane_send,
        plane_recv,
        att_send,
        att_recv,
        sum_send,
        sum_recv,
    ) = refs[2 * count + 2 :]
    devices = groups * seq_size
    group = lax.axis_index("grp")
    place = lax.axis_index("seq")
    me = group * seq_size + place
    rows, width = held["hidden"].shape
    model = devices * width
    own, window, _ = held["cached"].shape
    kv_width = held["w_key"].shape[1]
    q_width = held["w_query"].shape[1]
    kv_here = kv_width // HEAD_SIZE
    heads = q_width // HEAD_SIZE
    per_kv = heads // kv_here
    state_size = held["decay"].shape[0]

    def group_at(dg):
        return lax.rem(group + dg, groups) if dg else group

    def place_at(ds):
        return lax.rem(place + ds, seq_size) if ds else place

    every = [
        (dg * seq_size + ds, (group_at(dg), place_at(ds)))
        for dg in range(groups)
        for ds in range(seq_size)
        if dg or ds
    ]
    plane = [(ds, (group, place_at(ds))) for ds in range(1, seq_size)]
    column = [(dg, (group_at(dg), place)) for dg in range(1, groups)]

    def remote(src, dst, send, recv, k, where):
        return pltpu.make_async_remote_copy(
            src_ref=src,
            dst_ref=dst,
            send_sem=send.at[k],
            recv_sem=recv.at[k],
            device_id=where,
            device_id_type=MESH,
        )

    barrier = pltpu.get_barrier_semaphore()
    for _, where in every:
        pl.semaphore_signal(barrier, inc=1, device_id=where, device_id_type=MESH)

    def load(name):
        return pltpu.make_async_copy(
            hbm[name], held[name], in_sem.at[OPERANDS.index(name)]
        )

    tiles = window // tile

    def load_x(b, t):
        at = (b, pl.ds(t * tile, tile))
        return pltpu.make_async_copy(
            hbm["cached"].at[at], held["cached"].at[at], x_sem.at[b * tiles + t]
        )

    def start(*names):
        for name in names:
            load(name).start()

    def finish(*names):
        for name in names:
            load(name).wait()

    start("hidden", "w_key")
    load_x(0, 0).start()
    start("w_value", "cosine", "sine", "lengths")
    for t in range(1, tiles):
        load_x(0, t).start()
    start("gain", "conv_w", "conv_b", "conv_s")
    for b in range(1, own):
        for t in range(tiles):
            load_x(b, t).start()
    later = ["w_in", "w_state", "w_gate", "w_query", "w_step", "step_b", "decay", "skip"]
    last = ["m_gate", "m_up", "m_down", "state", "w_attn", "w_out"]

    finish("w_key", "cosine", "sine")

    def project(b, t):
        load_x(b, t).wait()
        x = held["cached"][b, t * tile : (t + 1) * tile, :]
        slots = slice(t * tile, (t + 1) * tile)
        at = slice(b * window + t * tile, b * window + (t + 1) * tile)
        k_rows = dot_nn(x, held["w_key"][...])
        cosine, sine = held["cosine"][slots, :], held["sine"][slots, :]
        for h in range(kv_here):
            cols = slice(h * HEAD_SIZE, (h + 1) * HEAD_SIZE)
            keys[at, cols] = turned(k_rows[:, cols], cosine, sine)
        if b == 0 and t == 0:
            finish("w_value")
        v_rows = dot_nn(x, held["w_value"][...])
        values[at, :] = v_rows.astype(bf16)

    gather = [(k, where, remote(held["hidden"], gathered.at[me], gather_send, gather_recv, k, where)) for k, where in every]

    for b in range(own):
        for t in range(tiles):
            project(b, t)
            if b == 0 and t == 0:
                finish("hidden")
                pl.semaphore_wait(barrier, devices - 1)
                for _, _, copy in gather:
                    copy.start()
                gathered[me] = held["hidden"][...]
                start(*later)
        if b == 0:
            start(*last)

    finish("gain", "conv_w", "conv_b", "conv_s")
    past = held["conv_b"][...]
    for k in range(held["conv_s"].shape[0]):
        past = past + held["conv_s"][k].astype(f32) * held["conv_w"][k : k + 1, :]
    conv_ref[...] = past

    for _, _, copy in gather:
        copy.wait()
    total = jnp.zeros((rows, width), f32)
    for d in range(devices):
        block = gathered[d].astype(f32)
        total = total + block * block
    scale = lax.rsqrt(jnp.sum(total, axis=1, keepdims=True) * (1.0 / model) + epsilon)
    for d in range(devices):
        cols = slice(d * width, (d + 1) * width)
        normed_ref[:, cols] = (gathered[d].astype(f32) * scale * held["gain"][:, cols]).astype(bf16)

    finish("w_in", "w_state")
    normed = normed_ref[...]
    taps = held["conv_w"].shape[0]
    ssm_input = dot_nn(normed, held["w_in"][...]).astype(bf16).astype(f32)
    conv_out = silu(conv_ref[...] + held["conv_w"][taps - 1 : taps, :] * ssm_input)
    conv_ref[...] = conv_out
    part_src[...] = dot_nt(conv_out.astype(bf16), held["w_state"][...]).astype(bf16)

    part = [remote(part_src, part_land.at[place], part_send, part_recv, k, where) for k, where in plane]
    for copy in part:
        copy.start()
    part_land[place] = part_src[...]

    finish("w_query", "w_gate", "lengths")
    query_rows[...] = dot_nn(normed, held["w_query"][...])
    key_rows[...] = dot_nn(normed, held["w_key"][...])
    value_rows[...] = dot_nn(normed, held["w_value"][...])
    gate_ref[...] = silu(dot_nn(normed, held["w_gate"][...]))

    first = place * own
    score_scale = HEAD_SIZE ** (-0.5)
    padded = -(-heads // 8) * 8
    row_id = lax.broadcasted_iota(jnp.int32, (padded, HEAD_SIZE), 0)
    slot_id = lax.broadcasted_iota(jnp.int32, (padded, window), 1)

    def attend(b):
        length = held["lengths"][first + b]
        q_row = query_rows[pl.ds(first + b, 1), :]
        k_row = key_rows[pl.ds(first + b, 1), :]
        v_row = value_rows[pl.ds(first + b, 1), :]
        cosine = held["cosine"][pl.ds(length, 1), :]
        sine = held["sine"][pl.ds(length, 1), :]
        stacked = jnp.zeros((padded, HEAD_SIZE), f32)
        for q in range(heads):
            stacked = jnp.where(row_id == q, q_row[:, q * HEAD_SIZE : (q + 1) * HEAD_SIZE], stacked)
        query = turned(stacked, cosine, sine).astype(f32)
        wide = jnp.concatenate(
            [
                jnp.where((row_id >= h * per_kv) & (row_id < (h + 1) * per_kv), query, 0.0)
                for h in range(kv_here)
            ],
            axis=1,
        )
        fresh_key = jnp.concatenate(
            [
                turned(k_row[:, h * HEAD_SIZE : (h + 1) * HEAD_SIZE], cosine, sine).astype(f32)
                for h in range(kv_here)
            ],
            axis=1,
        )
        here = slice(b * window, (b + 1) * window)
        scores = dot_nt(wide.astype(bf16), keys[here, :]) * score_scale
        scores = jnp.where(slot_id < length, scores, -1e30)
        fresh = jnp.sum(wide * fresh_key, axis=1, keepdims=True) * score_scale
        top = jnp.maximum(jnp.max(scores, axis=1, keepdims=True), fresh)
        weights = jnp.exp(scores - top)
        weight_new = jnp.exp(fresh - top)
        total = jnp.sum(weights, axis=1, keepdims=True) + weight_new
        mixed = dot_nn(weights.astype(bf16), values[here, :])
        mixed = (mixed + weight_new * v_row.astype(bf16).astype(f32)) / total
        mixed = mixed.astype(bf16).astype(f32)
        for q in range(heads):
            h = q // per_kv
            att_src[b : b + 1, q * HEAD_SIZE : (q + 1) * HEAD_SIZE] = mixed[
                q : q + 1, h * HEAD_SIZE : (h + 1) * HEAD_SIZE
            ]

    for b in range(own):
        attend(b)

    att = [remote(att_src, att_land.at[place], att_send, att_recv, k, where) for k, where in plane]
    for copy in part:
        copy.wait()
    plane_sum = part_land[0].astype(f32)
    for s in range(1, seq_size):
        plane_sum = plane_sum + part_land[s].astype(f32)
    plane_src[...] = plane_sum
    crossing = [
        remote(plane_src, plane_land.at[group], plane_send, plane_recv, k, where) for k, where in column
    ]
    for copy in crossing:
        copy.start()
    for copy in att:
        copy.start()
    plane_land[group] = plane_sum
    att_land[place] = att_src[...]

    finish("m_gate", "m_up")
    hidden = (
        silu(dot_nt(normed, held["m_gate"][...])) * dot_nt(normed, held["m_up"][...])
    ).astype(bf16)
    finish("m_down", "w_attn")
    term[...] = dot_nn(hidden, held["m_down"][...])
    finish("w_step", "step_b", "decay", "skip", "state", "w_out")
    rate = jnp.exp(held["decay"][...])

    for copy in crossing:
        copy.wait()
    low = plane_land[0]
    for z in range(1, groups):
        low = low + plane_land[z]
    low_ref[...] = low
    raw = dot_nn(low[:, :rank].astype(bf16), held["w_step"][...]) + held["step_b"][...]
    step_ref[...] = jnp.maximum(raw, 0.0) + jnp.log1p(jnp.exp(-jnp.abs(raw)))

    def advance(i, carry):
        some = pl.ds(pl.multiple_of(i * 8, 8), 8)
        step = step_ref[some, :][:, None, :]
        conv = conv_ref[some, :][:, None, :]
        tail = low_ref[some, :]
        input_map = tail[:, rank : rank + state_size][:, :, None]
        output_map = tail[:, rank + state_size :][:, :, None]
        fresh = jnp.exp(-step * rate[None]) * held["state"][some] + (step * conv) * input_map
        held["state"][some] = fresh
        mix_ref[some, :] = jnp.sum(fresh * output_map, axis=1)
        return carry

    lax.fori_loop(0, rows // 8, advance, 0)
    mixed = mix_ref[...] + held["skip"][...] * conv_ref[...]
    ssm_gated = (mixed * gate_ref[...]).astype(bf16)

    for copy in att:
        copy.wait()
    attended = jnp.concatenate([att_land[s] for s in range(seq_size)], axis=0).astype(bf16)
    col_width = held["w_attn"].shape[1]
    cols = pl.ds(pl.multiple_of(place * col_width, col_width), col_width)
    term[:, cols] += dot_nn(attended, held["w_attn"][...])

    save = pltpu.make_async_copy(held["state"], state_out_ref, out_sem)
    save.start()

    chunk = seq_size * width
    order = sorted(range(groups), key=lambda dg: -min(dg, groups - dg))

    def leave(dg, ds):
        where = (group_at(dg), place_at(ds))
        return remote(
            outgoing.at[where[0] * seq_size + where[1]],
            landed.at[me],
            sum_send,
            sum_recv,
            dg * seq_size + ds,
            where,
        )

    for dg in order:
        base = group_at(dg)
        cols = pl.ds(pl.multiple_of(base * chunk, chunk), chunk)
        block = dot_nn(ssm_gated, held["w_out"][:, cols]) + term[:, cols]
        for s in range(seq_size):
            outgoing[base * seq_size + s] = block[:, s * width : (s + 1) * width].astype(bf16)
        for ds in range(seq_size):
            if dg or ds:
                leave(dg, ds).start()
    landed[me] = outgoing[me]
    for k, _ in every:
        leave(k // seq_size, k % seq_size).wait()
    total = landed[0].astype(f32)
    for d in range(1, devices):
        total = total + landed[d].astype(f32)
    out_ref[...] = (held["hidden"][...].astype(f32) + total).astype(bf16)
    save.wait()


def rotary_tables(count):
    half_dim = HEAD_SIZE // 2
    frequency = rope_base ** (-(np.arange(half_dim, dtype=np.float32) * 2.0) / HEAD_SIZE)
    angles = np.arange(count, dtype=np.float32)[:, None] * frequency.astype(np.float32)
    cosine, sine = np.cos(angles), np.sin(angles)
    return (
        np.concatenate([cosine, cosine], axis=1).astype(np.float32),
        np.concatenate([-sine, sine], axis=1).astype(np.float32),
    )


def per_device(
    groups,
    seq_size,
    hidden_in,
    norm_gain,
    w_ssm_in,
    w_ssm_gate,
    conv_weight,
    conv_bias,
    conv_state,
    w_state_proj,
    w_step,
    step_bias,
    log_decay,
    skip_gain,
    ssm_state,
    w_ssm_out,
    w_query,
    key_projection,
    value_projection,
    w_attn_out,
    w_mlp_gate,
    w_mlp_up,
    w_mlp_down,
    cached_inputs,
    window_lengths,
):
    rows, width = hidden_in.shape
    devices = groups * seq_size
    model = devices * width
    own, window, _ = cached_inputs.shape
    kv_width, q_width = key_projection.shape[1], w_query.shape[1]
    channels = w_ssm_in.shape[1]
    low_width = w_state_proj.shape[1]
    tile = 256 if window % 256 == 0 else window
    cosine, sine = rotary_tables(window + 8)
    operands = dict(
        hidden=hidden_in,
        gain=norm_gain.reshape(1, -1),
        w_in=w_ssm_in,
        w_gate=w_ssm_gate,
        conv_w=conv_weight,
        conv_b=conv_bias.reshape(1, -1),
        conv_s=conv_state.transpose(1, 0, 2),
        w_state=w_state_proj.T,
        w_step=w_step,
        step_b=step_bias.reshape(1, -1),
        decay=log_decay,
        skip=skip_gain.reshape(1, -1),
        state=ssm_state,
        w_out=w_ssm_out,
        w_query=w_query,
        w_key=key_projection,
        w_value=value_projection,
        w_attn=w_attn_out,
        m_gate=w_mlp_gate.T,
        m_up=w_mlp_up.T,
        m_down=w_mlp_down,
        cached=cached_inputs,
        lengths=window_lengths,
        cosine=jnp.asarray(cosine),
        sine=jnp.asarray(sine),
    )
    dma = pltpu.SemaphoreType.DMA
    any_spec = pl.BlockSpec(memory_space=pl.ANY)
    own_copies = [
        (pltpu.SMEM if name == "lengths" else pltpu.VMEM)(operands[name].shape, operands[name].dtype)
        for name in OPERANDS
    ]
    return pl.pallas_call(
        functools.partial(step_kernel, groups, seq_size, w_step.shape[0], tile),
        out_shape=(
            jax.ShapeDtypeStruct((rows, width), bf16),
            jax.ShapeDtypeStruct(ssm_state.shape, f32),
        ),
        in_specs=[any_spec] * len(OPERANDS),
        out_specs=(pl.BlockSpec(memory_space=pltpu.VMEM), any_spec),
        scratch_shapes=own_copies
        + [
            pltpu.VMEM((devices, rows, width), bf16),
            pltpu.VMEM((rows, model), bf16),
            pltpu.VMEM((own * window, kv_width), bf16),
            pltpu.VMEM((own * window, kv_width), bf16),
            pltpu.VMEM((rows, q_width), f32),
            pltpu.VMEM((rows, kv_width), f32),
            pltpu.VMEM((rows, kv_width), f32),
            pltpu.VMEM((rows, low_width), bf16),
            pltpu.VMEM((seq_size, rows, low_width), bf16),
            pltpu.VMEM((rows, low_width), f32),
            pltpu.VMEM((groups, rows, low_width), f32),
            pltpu.VMEM((rows, low_width), f32),
            pltpu.VMEM((rows, channels), f32),
            pltpu.VMEM((rows, channels), f32),
            pltpu.VMEM((rows, channels), f32),
            pltpu.VMEM((rows, channels), f32),
            pltpu.VMEM((own, q_width), f32),
            pltpu.VMEM((seq_size, own, q_width), f32),
            pltpu.VMEM((rows, model), f32),
            pltpu.VMEM((devices, rows, width), bf16),
            pltpu.VMEM((devices, rows, width), bf16),
            dma((len(OPERANDS),)),
            dma((own * window // tile,)),
            dma,
            dma((devices,)),
            dma((devices,)),
            dma((seq_size,)),
            dma((seq_size,)),
            dma((groups,)),
            dma((groups,)),
            dma((seq_size,)),
            dma((seq_size,)),
            dma((devices,)),
            dma((devices,)),
        ],
        compiler_params=pltpu.CompilerParams(
            collective_id=0, has_side_effects=True, vmem_limit_bytes=VMEM_LIMIT
        ),
    )(*[operands[name] for name in OPERANDS])


def solution(mesh):
    placed = (
        P(None, ("grp", "seq")),
        P(),
        P(None, ("grp", "seq")),
        P(None, ("grp", "seq")),
        P(None, ("grp", "seq")),
        P(("grp", "seq")),
        P(None, None, ("grp", "seq")),
        P(("grp", "seq"), None),
        P(None, ("grp", "seq")),
        P(("grp", "seq")),
        P(None, ("grp", "seq")),
        P(("grp", "seq")),
        P(None, None, ("grp", "seq")),
        P(("grp", "seq"), None),
        P(None, "grp"),
        P(None, "grp"),
        P(None, "grp"),
        P("grp", "seq"),
        P(None, ("grp", "seq")),
        P(None, ("grp", "seq")),
        P(("grp", "seq"), None),
        P("seq", None, None),
        P(),
    )
    return jax.shard_map(
        functools.partial(per_device, mesh.shape["grp"], mesh.shape["seq"]),
        mesh=mesh,
        in_specs=placed,
        out_specs=(P(None, ("grp", "seq")), P(None, None, ("grp", "seq"))),
        check_vma=False,
    )
```

```python
import functools

import jax
import jax.numpy as jnp
import numpy as np
from jax import lax
from jax.experimental import pallas as pl
from jax.experimental.pallas import tpu as pltpu
from jax.sharding import PartitionSpec as P

HEAD_SIZE = 128
MESH = pl.DeviceIdType.MESH
VMEM_LIMIT = 48 * 1024 * 1024
LATE = 1
MEET_LAST = 2

epsilon = 1e-05
rope_base = 10000.0

bf16 = jnp.bfloat16
f32 = jnp.float32


def dot_nn(a, b):
    return jnp.dot(a, b, preferred_element_type=f32)


def dot_nt(a, b):
    return lax.dot_general(a, b, (((1,), (1,)), ((), ())), preferred_element_type=f32)


def dot_halves(a, b):
    half = b.shape[0] // 2
    return dot_nn(a[:, :half], b[:half, :]) + dot_nn(a[:, half:], b[half:, :])


def silu(v):
    return v / (1.0 + jnp.exp(-v))


def turned(values, cosine, sine):
    return (values * cosine + pltpu.roll(values, HEAD_SIZE // 2, 1) * sine).astype(bf16)


OPERANDS = (
    "hidden",
    "gain",
    "w_in",
    "w_gate",
    "conv_w",
    "conv_b",
    "conv_s",
    "w_state",
    "w_step",
    "step_b",
    "decay",
    "skip",
    "state",
    "w_out",
    "w_query",
    "w_key",
    "w_value",
    "w_attn",
    "m_gate",
    "m_up",
    "m_down",
    "cached",
    "lengths",
    "cosine",
    "sine",
)


def step_kernel(groups, seq_size, rank, tile, *refs):
    count = len(OPERANDS)
    hbm = dict(zip(OPERANDS, refs[:count]))
    out_ref, state_out_ref = refs[count : count + 2]
    held = dict(zip(OPERANDS, refs[count + 2 : 2 * count + 2]))
    (
        gathered,
        normed_ref,
        keys,
        values,
        query_rows,
        key_rows,
        value_rows,
        part_src,
        part_land,
        plane_src,
        plane_land,
        low_ref,
        step_ref,
        conv_ref,
        mix_ref,
        gate_ref,
        att_src,
        att_land,
        term,
        outgoing,
        landed,
        in_sem,
        x_sem,
        link_sem,
    ) = refs[2 * count + 2 :]
    devices = groups * seq_size
    group = lax.axis_index("grp")
    place = lax.axis_index("seq")
    me = group * seq_size + place
    rows, width = held["hidden"].shape
    model = devices * width
    own, window, _ = held["cached"].shape
    kv_width = held["w_key"].shape[1]
    q_width = held["w_query"].shape[1]
    kv_here = kv_width // HEAD_SIZE
    heads = q_width // HEAD_SIZE
    per_kv = heads // kv_here
    state_size = held["decay"].shape[0]

    def group_at(dg):
        return lax.rem(group + dg, groups) if dg else group

    def place_at(ds):
        return lax.rem(place + ds, seq_size) if ds else place

    every = [
        (dg * seq_size + ds, (group_at(dg), place_at(ds)))
        for dg in range(groups)
        for ds in range(seq_size)
        if dg or ds
    ]
    plane = [(ds, (group, place_at(ds))) for ds in range(1, seq_size)]
    column = [(dg, (group_at(dg), place)) for dg in range(1, groups)]

    def remote(src, dst, pair, where):
        return pltpu.make_async_remote_copy(
            src_ref=src,
            dst_ref=dst,
            send_sem=link_sem.at[2 * pair],
            recv_sem=link_sem.at[2 * pair + 1],
            device_id=where,
            device_id_type=MESH,
        )

    def await_sent(block, pair):
        pltpu.make_async_copy(block, block, link_sem.at[2 * pair]).wait()

    def await_landed(block, pair):
        pltpu.make_async_copy(block, block, link_sem.at[2 * pair + 1]).wait()

    barrier = pltpu.get_barrier_semaphore()
    for _, where in every:
        pl.semaphore_signal(barrier, inc=1, device_id=where, device_id_type=MESH)

    def load(name):
        return pltpu.make_async_copy(
            hbm[name], held[name], in_sem.at[OPERANDS.index(name)]
        )

    tiles = window // tile

    def load_x(b, t):
        at = (b, pl.ds(t * tile, tile))
        return pltpu.make_async_copy(
            hbm["cached"].at[at], held["cached"].at[at], x_sem.at[b * tiles + t]
        )

    def start(*names):
        for name in names:
            load(name).start()

    def finish(*names):
        for name in names:
            load(name).wait()

    spans = [(b, t) for b in range(own) for t in range(tiles)]
    waiting = [
        ["gain", "conv_w", "conv_b", "conv_s", "lengths"],
        ["w_in", "w_state"],
        ["w_query", "w_gate"],
        ["m_gate"],
        ["m_up", "w_step", "step_b", "decay", "skip"],
        ["m_down", "state", "w_attn", "w_out"],
    ]
    start("hidden", "w_key")
    load_x(*spans[0]).start()
    start("w_value", "cosine", "sine")

    def meet():
        with jax.named_scope("meet"):
            finish("hidden")
            pl.semaphore_wait(barrier, devices - 1)
        for _, where in every:
            remote(held["hidden"], gathered.at[me], 0, where).start()
        gathered[me] = held["hidden"][...]

    far = group == groups - 1
    first_chip = jnp.logical_and(group == 0, place < 2)
    middle = jnp.logical_not(jnp.logical_or(far, first_chip))
    pl.when(far)(meet)
    with jax.named_scope("first_wait"):
        finish("w_key")

    load_x(*spans[1]).start()

    def project(i):
        b, t = spans[i]
        load_x(b, t).wait()
        if i == 0:
            finish("w_value", "cosine", "sine")
        if i + 2 < len(spans):
            load_x(*spans[i + 2]).start()
        last = len(waiting) if i + 1 == len(spans) else i + 1
        for names in waiting[i:last]:
            start(*names)
        x = held["cached"][b, t * tile : (t + 1) * tile, :]
        slots = slice(t * tile, (t + 1) * tile)
        at = slice(b * window + t * tile, b * window + (t + 1) * tile)
        k_rows = dot_nn(x, held["w_key"][...])
        cosine, sine = held["cosine"][slots, :], held["sine"][slots, :]
        for h in range(kv_here):
            cols = slice(h * HEAD_SIZE, (h + 1) * HEAD_SIZE)
            keys[at, cols] = turned(k_rows[:, cols], cosine, sine)
        v_rows = dot_nn(x, held["w_value"][...])
        values[at, :] = v_rows.astype(bf16)


    early = max(len(spans) - LATE, 1)
    for i in range(early):
        with jax.named_scope("project"):
            project(i)
        if i == 0:
            pl.when(middle)(meet)
        if i == min(early - 1, MEET_LAST):
            pl.when(first_chip)(meet)

    finish("gain", "conv_w", "conv_b", "conv_s")
    past = held["conv_b"][...]
    for k in range(held["conv_s"].shape[0]):
        past = past + held["conv_s"][k].astype(f32) * held["conv_w"][k : k + 1, :]
    conv_ref[...] = past

    with jax.named_scope("gather_wait"):
        await_landed(gathered.at[pl.ds(0, devices - 1)], 0)

    with jax.named_scope("norm"):
        total = jnp.zeros((rows, width), f32)
        for d in range(devices):
            block = gathered[d].astype(f32)
            total = total + block * block
        scale = lax.rsqrt(jnp.sum(total, axis=1, keepdims=True) * (1.0 / model) + epsilon)
        for d in range(devices):
            cols = slice(d * width, (d + 1) * width)
            normed_ref[:, cols] = (gathered[d].astype(f32) * scale * held["gain"][:, cols]).astype(bf16)

    with jax.named_scope("ssm_in"):
        finish("w_in", "w_state")
        normed = normed_ref[...]
        taps = held["conv_w"].shape[0]
        ssm_input = dot_halves(normed, held["w_in"][...]).astype(bf16).astype(f32)
        conv_out = silu(conv_ref[...] + held["conv_w"][taps - 1 : taps, :] * ssm_input)
        conv_ref[...] = conv_out
        part_src[...] = dot_nt(conv_out.astype(bf16), held["w_state"][...]).astype(bf16)

    for _, where in plane:
        remote(part_src, part_land.at[place], 1, where).start()
    part_land[place] = part_src[...]

    for i in range(early, len(spans)):
        with jax.named_scope("project"):
            project(i)
    with jax.named_scope("qkv_gate"):
        finish("w_query", "w_gate", "lengths")
        query_rows[...] = dot_nn(normed, held["w_query"][...])
        key_rows[...] = dot_nn(normed, held["w_key"][...])
        value_rows[...] = dot_nn(normed, held["w_value"][...])
        gate_ref[...] = silu(dot_nn(normed, held["w_gate"][...]))

    first = place * own
    score_scale = HEAD_SIZE ** (-0.5)
    padded = -(-heads // 8) * 8
    row_id = lax.broadcasted_iota(jnp.int32, (padded, HEAD_SIZE), 0)
    slot_id = lax.broadcasted_iota(jnp.int32, (padded, window), 1)

    def attend(b):
        length = held["lengths"][first + b]
        q_row = query_rows[pl.ds(first + b, 1), :]
        k_row = key_rows[pl.ds(first + b, 1), :]
        v_row = value_rows[pl.ds(first + b, 1), :]
        cosine = held["cosine"][pl.ds(length, 1), :]
        sine = held["sine"][pl.ds(length, 1), :]
        stacked = jnp.zeros((padded, HEAD_SIZE), f32)
        for q in range(heads):
            stacked = jnp.where(row_id == q, q_row[:, q * HEAD_SIZE : (q + 1) * HEAD_SIZE], stacked)
        query = turned(stacked, cosine, sine).astype(f32)
        wide = jnp.concatenate(
            [
                jnp.where((row_id >= h * per_kv) & (row_id < (h + 1) * per_kv), query, 0.0)
                for h in range(kv_here)
            ],
            axis=1,
        )
        fresh_key = jnp.concatenate(
            [
                turned(k_row[:, h * HEAD_SIZE : (h + 1) * HEAD_SIZE], cosine, sine).astype(f32)
                for h in range(kv_here)
            ],
            axis=1,
        )
        here = slice(b * window, (b + 1) * window)
        scores = dot_nt(wide.astype(bf16), keys[here, :]) * score_scale
        scores = jnp.where(slot_id < length, scores, -1e30)
        fresh = jnp.sum(wide * fresh_key, axis=1, keepdims=True) * score_scale
        top = jnp.maximum(jnp.max(scores, axis=1, keepdims=True), fresh)
        weights = jnp.exp(scores - top)
        weight_new = jnp.exp(fresh - top)
        total = jnp.sum(weights, axis=1, keepdims=True) + weight_new
        mixed = dot_nn(weights.astype(bf16), values[here, :])
        mixed = (mixed + weight_new * v_row.astype(bf16).astype(f32)) / total
        mixed = mixed.astype(bf16).astype(f32)
        for q in range(heads):
            h = q // per_kv
            att_src[b : b + 1, q * HEAD_SIZE : (q + 1) * HEAD_SIZE] = mixed[
                q : q + 1, h * HEAD_SIZE : (h + 1) * HEAD_SIZE
            ]

    with jax.named_scope("attend"):
        for b in range(own):
            attend(b)

    with jax.named_scope("part_wait"):
        await_landed(part_land.at[pl.ds(0, seq_size - 1)], 1)

    plane_sum = part_land[0].astype(f32)
    for s in range(1, seq_size):
        plane_sum = plane_sum + part_land[s].astype(f32)
    plane_src[...] = plane_sum.astype(bf16)
    for _, where in column:
        remote(plane_src, plane_land.at[group], 2, where).start()
    for _, where in plane:
        remote(att_src, att_land.at[place], 3, where).start()
    plane_land[group] = plane_src[...]
    att_land[place] = att_src[...]

    with jax.named_scope("mlp"):
        finish("m_gate", "m_up")
        hidden = (
            silu(dot_nt(normed, held["m_gate"][...])) * dot_nt(normed, held["m_up"][...])
        ).astype(bf16)
        finish("m_down", "w_attn")
        term[...] = dot_nn(hidden, held["m_down"][...])

    finish("w_step", "step_b", "decay", "skip", "state", "w_out")
    rate = jnp.exp(held["decay"][...])

    with jax.named_scope("cross_wait"):
        await_landed(plane_land.at[pl.ds(0, groups - 1)], 2)

    with jax.named_scope("step_size"):
        low = plane_land[0].astype(f32)
        for z in range(1, groups):
            low = low + plane_land[z].astype(f32)
        low_ref[...] = low
        raw = dot_nn(low[:, :rank].astype(bf16), held["w_step"][...]) + held["step_b"][...]
        step_ref[...] = jnp.maximum(raw, 0.0) + jnp.log1p(jnp.exp(-jnp.abs(raw)))

    def advance(i, carry):
        some = pl.ds(pl.multiple_of(i * 8, 8), 8)
        step = step_ref[some, :][:, None, :]
        conv = conv_ref[some, :][:, None, :]
        tail = low_ref[some, :]
        input_map = tail[:, rank : rank + state_size][:, :, None]
        output_map = tail[:, rank + state_size :][:, :, None]
        fresh = jnp.exp(-step * rate[None]) * held["state"][some] + (step * conv) * input_map
        state_out_ref[some] = fresh
        mix_ref[some, :] = jnp.sum(fresh * output_map, axis=1)
        return carry

    with jax.named_scope("advance"):
        lax.fori_loop(0, rows // 8, advance, 0)
        mixed = mix_ref[...] + held["skip"][...] * conv_ref[...]
        ssm_gated = (mixed * gate_ref[...]).astype(bf16)

    with jax.named_scope("att_wait"):
        await_landed(att_land.at[pl.ds(0, seq_size - 1)], 3)

    with jax.named_scope("attn_out"):
        attended = jnp.concatenate([att_land[s] for s in range(seq_size)], axis=0).astype(bf16)
        col_width = held["w_attn"].shape[1]
        cols = pl.ds(pl.multiple_of(place * col_width, col_width), col_width)
        term[:, cols] += dot_nn(attended, held["w_attn"][...])

    chunk = seq_size * width
    order = sorted(range(groups), key=lambda dg: -min(dg, groups - dg))

    def leave(dg, ds):
        where = (group_at(dg), place_at(ds))
        return remote(
            outgoing.at[where[0] * seq_size + where[1]],
            landed.at[me],
            4,
            where,
        )

    with jax.named_scope("ssm_out"):
        for dg in order:
            base = group_at(dg)
            cols = pl.ds(pl.multiple_of(base * chunk, chunk), chunk)
            block = dot_nn(ssm_gated, held["w_out"][:, cols]) + term[:, cols]
            for s in range(seq_size):
                outgoing[base * seq_size + s] = block[:, s * width : (s + 1) * width].astype(bf16)
            for ds in range(seq_size):
                if dg or ds:
                    leave(dg, ds).start()

    landed[me] = outgoing[me]
    with jax.named_scope("sum_wait"):
        await_landed(landed.at[pl.ds(0, devices - 1)], 4)

    with jax.named_scope("final"):
        total = landed[0].astype(f32)
        for d in range(1, devices):
            total = total + landed[d].astype(f32)
        out_ref[...] = (held["hidden"][...].astype(f32) + total).astype(bf16)
    await_sent(gathered.at[pl.ds(0, devices - 1)], 0)
    await_sent(part_land.at[pl.ds(0, seq_size - 1)], 1)
    await_sent(plane_land.at[pl.ds(0, groups - 1)], 2)
    await_sent(att_land.at[pl.ds(0, seq_size - 1)], 3)
    await_sent(landed.at[pl.ds(0, devices - 1)], 4)


def store_kernel(hidden_ref, state_ref, hidden_out, state_out, sem):
    copies = [
        pltpu.make_async_copy(state_ref, state_out, sem.at[0]),
        pltpu.make_async_copy(hidden_ref, hidden_out, sem.at[1]),
    ]
    for copy in copies:
        copy.start()
    for copy in copies:
        copy.wait()


def rotary_tables(count):
    half_dim = HEAD_SIZE // 2
    frequency = rope_base ** (-(np.arange(half_dim, dtype=np.float32) * 2.0) / HEAD_SIZE)
    angles = np.arange(count, dtype=np.float32)[:, None] * frequency.astype(np.float32)
    cosine, sine = np.cos(angles), np.sin(angles)
    return (
        np.concatenate([cosine, cosine], axis=1).astype(np.float32),
        np.concatenate([-sine, sine], axis=1).astype(np.float32),
    )


def per_device(
    groups,
    seq_size,
    hidden_in,
    norm_gain,
    w_ssm_in,
    w_ssm_gate,
    conv_weight,
    conv_bias,
    conv_state,
    w_state_proj,
    w_step,
    step_bias,
    log_decay,
    skip_gain,
    ssm_state,
    w_ssm_out,
    w_query,
    key_projection,
    value_projection,
    w_attn_out,
    w_mlp_gate,
    w_mlp_up,
    w_mlp_down,
    cached_inputs,
    window_lengths,
):
    rows, width = hidden_in.shape
    devices = groups * seq_size
    model = devices * width
    own, window, _ = cached_inputs.shape
    kv_width, q_width = key_projection.shape[1], w_query.shape[1]
    channels = w_ssm_in.shape[1]
    low_width = w_state_proj.shape[1]
    tile = 256 if window % 256 == 0 else window
    cosine, sine = rotary_tables(window + 8)
    operands = dict(
        hidden=hidden_in,
        gain=norm_gain.reshape(1, -1),
        w_in=w_ssm_in,
        w_gate=w_ssm_gate,
        conv_w=conv_weight,
        conv_b=conv_bias.reshape(1, -1),
        conv_s=conv_state.transpose(1, 0, 2),
        w_state=w_state_proj.T,
        w_step=w_step,
        step_b=step_bias.reshape(1, -1),
        decay=log_decay,
        skip=skip_gain.reshape(1, -1),
        state=ssm_state,
        w_out=w_ssm_out,
        w_query=w_query,
        w_key=key_projection,
        w_value=value_projection,
        w_attn=w_attn_out,
        m_gate=w_mlp_gate.T,
        m_up=w_mlp_up.T,
        m_down=w_mlp_down,
        cached=cached_inputs,
        lengths=window_lengths,
        cosine=jnp.asarray(cosine),
        sine=jnp.asarray(sine),
    )
    dma = pltpu.SemaphoreType.DMA
    hbm_spec = pl.BlockSpec(memory_space=pltpu.HBM)
    vmem_spec = pl.BlockSpec(memory_space=pltpu.VMEM)
    own_copies = [
        (pltpu.SMEM if name == "lengths" else pltpu.VMEM)(operands[name].shape, operands[name].dtype)
        for name in OPERANDS
    ]
    hidden_out, state_out = pl.pallas_call(
        functools.partial(step_kernel, groups, seq_size, w_step.shape[0], tile),
        out_shape=(
            jax.ShapeDtypeStruct((rows, width), bf16),
            jax.ShapeDtypeStruct(ssm_state.shape, f32),
        ),
        in_specs=[hbm_spec] * len(OPERANDS),
        out_specs=(vmem_spec, vmem_spec),
        scratch_shapes=own_copies
        + [
            pltpu.VMEM((devices, rows, width), bf16),
            pltpu.VMEM((rows, model), bf16),
            pltpu.VMEM((own * window, kv_width), bf16),
            pltpu.VMEM((own * window, kv_width), bf16),
            pltpu.VMEM((rows, q_width), f32),
            pltpu.VMEM((rows, kv_width), f32),
            pltpu.VMEM((rows, kv_width), f32),
            pltpu.VMEM((rows, low_width), bf16),
            pltpu.VMEM((seq_size, rows, low_width), bf16),
            pltpu.VMEM((rows, low_width), bf16),
            pltpu.VMEM((groups, rows, low_width), bf16),
            pltpu.VMEM((rows, low_width), f32),
            pltpu.VMEM((rows, channels), f32),
            pltpu.VMEM((rows, channels), f32),
            pltpu.VMEM((rows, channels), f32),
            pltpu.VMEM((rows, channels), f32),
            pltpu.VMEM((own, q_width), f32),
            pltpu.VMEM((seq_size, own, q_width), f32),
            pltpu.VMEM((rows, model), f32),
            pltpu.VMEM((devices, rows, width), bf16),
            pltpu.VMEM((devices, rows, width), bf16),
            dma((len(OPERANDS),)),
            dma((own * window // tile,)),
            dma((10,)),
        ],
        compiler_params=pltpu.CompilerParams(
            collective_id=0, has_side_effects=True, vmem_limit_bytes=VMEM_LIMIT
        ),
    )(*[pltpu.with_memory_space_constraint(operands[name], pltpu.HBM) for name in OPERANDS])
    return pl.pallas_call(
        store_kernel,
        out_shape=(
            jax.ShapeDtypeStruct((rows, width), bf16),
            jax.ShapeDtypeStruct(ssm_state.shape, f32),
        ),
        in_specs=[vmem_spec] * 2,
        out_specs=(hbm_spec, hbm_spec),
        scratch_shapes=[dma((2,))],
        compiler_params=pltpu.CompilerParams(vmem_limit_bytes=1024 * 1024),
    )(hidden_out, state_out)


def solution(mesh):
    placed = (
        P(None, ("grp", "seq")),
        P(),
        P(None, ("grp", "seq")),
        P(None, ("grp", "seq")),
        P(None, ("grp", "seq")),
        P(("grp", "seq")),
        P(None, None, ("grp", "seq")),
        P(("grp", "seq"), None),
        P(None, ("grp", "seq")),
        P(("grp", "seq")),
        P(None, ("grp", "seq")),
        P(("grp", "seq")),
        P(None, None, ("grp", "seq")),
        P(("grp", "seq"), None),
        P(None, "grp"),
        P(None, "grp"),
        P(None, "grp"),
        P("grp", "seq"),
        P(None, ("grp", "seq")),
        P(None, ("grp", "seq")),
        P(("grp", "seq"), None),
        P("seq", None, None),
        P(),
    )
    return jax.shard_map(
        functools.partial(per_device, mesh.shape["grp"], mesh.shape["seq"]),
        mesh=mesh,
        in_specs=placed,
        out_specs=(P(None, ("grp", "seq")), P(None, None, ("grp", "seq"))),
        check_vma=False,
    )
```

```python
import functools

import jax
import jax.numpy as jnp
import numpy as np
from jax import lax
from jax.experimental import pallas as pl
from jax.experimental.pallas import tpu as pltpu
from jax.sharding import PartitionSpec as P

HEAD_SIZE = 128
MESH = pl.DeviceIdType.MESH
VMEM_LIMIT = 48 * 1024 * 1024
LATE = 1
MEET_LAST = 3
AHEAD = 4
PAIR = 2


def GATHER_ORDER(groups):
    return list(range(groups))


epsilon = 1e-05
rope_base = 10000.0

bf16 = jnp.bfloat16
f32 = jnp.float32


def dot_nn(a, b):
    return jnp.dot(a, b, preferred_element_type=f32)


def dot_nt(a, b):
    return lax.dot_general(a, b, (((1,), (1,)), ((), ())), preferred_element_type=f32)


def row_spans(own, window, tile):
    spans = [(b, at, tile) for b in range(own) for at in range(0, window, tile)]
    if tile % 2 == 0:
        b, at, size = spans[0]
        spans[:1] = [(b, at, size // 2), (b, at + size // 2, size // 2)]
    return spans


def silu(v):
    return v / (1.0 + jnp.exp(-v))


def turned(values, cosine, sine):
    return (values * cosine + pltpu.roll(values, HEAD_SIZE // 2, 1) * sine).astype(bf16)


OPERANDS = (
    "hidden",
    "gain",
    "w_in",
    "w_gate",
    "conv_w",
    "conv_b",
    "conv_s",
    "w_state",
    "w_step",
    "step_b",
    "decay",
    "skip",
    "state",
    "w_out",
    "w_query",
    "w_key",
    "w_value",
    "w_attn",
    "m_gate",
    "m_up",
    "m_down",
    "cached",
    "lengths",
    "cosine",
    "sine",
)


def step_kernel(groups, seq_size, rank, tile, *refs):
    count = len(OPERANDS)
    hbm = dict(zip(OPERANDS, refs[:count]))
    out_ref, state_out_ref = refs[count : count + 2]
    held = dict(zip(OPERANDS, refs[count + 2 : 2 * count + 2]))
    (
        gathered,
        normed_ref,
        keys,
        values,
        query_rows,
        key_rows,
        value_rows,
        part_src,
        part_land,
        plane_src,
        plane_land,
        low_ref,
        step_ref,
        conv_ref,
        mix_ref,
        gate_ref,
        att_src,
        att_land,
        term,
        outgoing,
        landed,
        halves_ref,
        in_sem,
        x_sem,
        link_sem,
    ) = refs[2 * count + 2 :]
    devices = groups * seq_size
    group = lax.axis_index("grp")
    place = lax.axis_index("seq")
    me = group * seq_size + place
    rows, width = held["hidden"].shape
    model = devices * width
    own, window, _ = held["cached"].shape
    kv_width = held["w_key"].shape[1]
    q_width = held["w_query"].shape[1]
    kv_here = kv_width // HEAD_SIZE
    heads = q_width // HEAD_SIZE
    per_kv = heads // kv_here
    state_size = held["decay"].shape[0]

    def group_at(dg):
        return lax.rem(group + dg, groups) if dg else group

    def place_at(ds):
        return lax.rem(place + ds, seq_size) if ds else place

    every = [
        (dg * seq_size + ds, (group_at(dg), place_at(ds)))
        for dg in GATHER_ORDER(groups)
        for ds in range(seq_size)
        if dg or ds
    ]
    plane = [(ds, (group, place_at(ds))) for ds in range(1, seq_size)]
    column = [(dg, (group_at(dg), place)) for dg in range(1, groups)]

    def remote(src, dst, pair, where):
        return pltpu.make_async_remote_copy(
            src_ref=src,
            dst_ref=dst,
            send_sem=link_sem.at[2 * pair],
            recv_sem=link_sem.at[2 * pair + 1],
            device_id=where,
            device_id_type=MESH,
        )

    def await_sent(block, pair):
        pltpu.make_async_copy(block, block, link_sem.at[2 * pair]).wait()

    def await_landed(block, pair):
        pltpu.make_async_copy(block, block, link_sem.at[2 * pair + 1]).wait()

    barrier = pltpu.get_barrier_semaphore()
    for _, where in every:
        pl.semaphore_signal(barrier, inc=1, device_id=where, device_id_type=MESH)

    def load(name):
        return pltpu.make_async_copy(
            hbm[name], held[name], in_sem.at[OPERANDS.index(name)]
        )

    spans = row_spans(own, window, tile)

    def load_x(i):
        b, at, size = spans[i]
        part = (b, pl.ds(at, size))
        return pltpu.make_async_copy(
            hbm["cached"].at[part], held["cached"].at[part], x_sem.at[i]
        )

    def start(*names):
        for name in names:
            load(name).start()

    def finish(*names):
        for name in names:
            load(name).wait()

    waiting = [
        [],
        [],
        ["gain", "conv_w", "conv_b", "conv_s", "lengths"],
        ["w_in", "w_state"],
        ["w_query", "w_gate"],
        ["m_gate", "m_up", "w_step", "step_b", "decay", "skip"],
        ["m_down", "state", "w_attn", "w_out"],
    ]
    start("hidden", "w_key")
    load_x(0).start()
    start("w_value", "cosine", "sine")
    load_x(1).start()

    def meet():
        with jax.named_scope("meet"):
            finish("hidden")
            pl.semaphore_wait(barrier, devices - 1)
        for n in range(groups):
            z = jnp.where(2 * group < groups, groups - 1 - n, n)
            for ds in range(seq_size):
                def go():
                    remote(held["hidden"], gathered.at[me], 0, (z, place_at(ds))).start()
                if ds:
                    go()
                else:
                    pl.when(z != group)(go)
        gathered[me] = held["hidden"][...]

    far = group >= groups // 2
    first_chip = jnp.logical_and(group == 0, place < 2)
    middle = jnp.logical_not(jnp.logical_or(far, first_chip))
    pl.when(far)(meet)
    with jax.named_scope("first_wait"):
        finish("w_key")

    ahead = min(AHEAD, len(spans))
    for n in range(2, ahead):
        load_x(n).start()

    def ready(i):
        load_x(i).wait()
        if i == 0:
            finish("w_value", "cosine", "sine")
        if i + ahead < len(spans):
            load_x(i + ahead).start()
        last = len(waiting) if i + 1 == len(spans) else i + 1
        for names in waiting[i:last]:
            start(*names)

    def project(i):
        b, begin, size = spans[i]
        slots = slice(begin, begin + size)
        x = held["cached"][b, slots, :]
        at = slice(b * window + begin, b * window + begin + size)
        k_rows = dot_nn(x, held["w_key"][...])
        cosine, sine = held["cosine"][slots, :], held["sine"][slots, :]
        for h in range(kv_here):
            cols = slice(h * HEAD_SIZE, (h + 1) * HEAD_SIZE)
            keys[at, cols] = turned(k_rows[:, cols], cosine, sine)
        v_rows = dot_nn(x, held["w_value"][...])
        values[at, :] = v_rows.astype(bf16)


    early = max(len(spans) - LATE, 1)
    i = 0
    while i < early:
        some = range(i, min(early, i + (PAIR if i else 1)))
        for n in some:
            ready(n)
        with jax.named_scope("project"):
            for n in some:
                project(n)
        if i == 0:
            pl.when(middle)(meet)
        i = some[-1] + 1
        if some[0] <= MEET_LAST < i or (i == early and MEET_LAST >= i):
            pl.when(first_chip)(meet)

    finish("gain", "conv_w", "conv_b", "conv_s", "w_in", "w_state")
    past = held["conv_b"][...]
    for k in range(held["conv_s"].shape[0]):
        past = past + held["conv_s"][k].astype(f32) * held["conv_w"][k : k + 1, :]
    conv_ref[...] = past

    with jax.named_scope("gather_wait"):
        await_landed(gathered.at[pl.ds(0, devices - 1)], 0)

    with jax.named_scope("norm"):
        total = jnp.zeros((rows, width), f32)
        for d in range(devices):
            block = gathered[d].astype(f32)
            total = total + block * block
        scale = lax.rsqrt(jnp.sum(total, axis=1, keepdims=True) * (1.0 / model) + epsilon)
        for d in range(devices):
            cols = slice(d * width, (d + 1) * width)
            normed_ref[:, cols] = (gathered[d].astype(f32) * scale * held["gain"][:, cols]).astype(bf16)

    with jax.named_scope("ssm_in"):
        normed = normed_ref[...]
        taps = held["conv_w"].shape[0]
        k_half = model // 2
        halves_ref[0] = dot_nn(normed[:, :k_half], held["w_in"][:k_half, :])
        halves_ref[1] = dot_nn(normed[:, k_half:], held["w_in"][k_half:, :])
        ssm_input = (halves_ref[0] + halves_ref[1]).astype(bf16).astype(f32)
        conv_out = silu(conv_ref[...] + held["conv_w"][taps - 1 : taps, :] * ssm_input)
        conv_ref[...] = conv_out
        part_src[...] = dot_nt(conv_out.astype(bf16), held["w_state"][...]).astype(bf16)

    for _, where in plane:
        remote(part_src, part_land.at[place], 1, where).start()
    part_land[place] = part_src[...]

    for i in range(early, len(spans)):
        ready(i)
    finish("w_query", "w_gate", "lengths")
    with jax.named_scope("qkv_gate"):
        for i in range(early, len(spans)):
            project(i)
        query_rows[...] = dot_nn(normed, held["w_query"][...])
        key_rows[...] = dot_nn(normed, held["w_key"][...])
        value_rows[...] = dot_nn(normed, held["w_value"][...])
        gate_ref[...] = silu(dot_nn(normed, held["w_gate"][...]))

    first = place * own
    score_scale = HEAD_SIZE ** (-0.5)
    padded = -(-heads // 8) * 8
    row_id = lax.broadcasted_iota(jnp.int32, (padded, HEAD_SIZE), 0)
    slot_id = lax.broadcasted_iota(jnp.int32, (padded, window), 1)

    def attend(b):
        length = held["lengths"][first + b]
        q_row = query_rows[pl.ds(first + b, 1), :]
        k_row = key_rows[pl.ds(first + b, 1), :]
        v_row = value_rows[pl.ds(first + b, 1), :]
        cosine = held["cosine"][pl.ds(length, 1), :]
        sine = held["sine"][pl.ds(length, 1), :]
        stacked = jnp.zeros((padded, HEAD_SIZE), f32)
        for q in range(heads):
            stacked = jnp.where(row_id == q, q_row[:, q * HEAD_SIZE : (q + 1) * HEAD_SIZE], stacked)
        query = turned(stacked, cosine, sine).astype(f32)
        wide = jnp.concatenate(
            [
                jnp.where((row_id >= h * per_kv) & (row_id < (h + 1) * per_kv), query, 0.0)
                for h in range(kv_here)
            ],
            axis=1,
        )
        fresh_key = jnp.concatenate(
            [
                turned(k_row[:, h * HEAD_SIZE : (h + 1) * HEAD_SIZE], cosine, sine).astype(f32)
                for h in range(kv_here)
            ],
            axis=1,
        )
        here = slice(b * window, (b + 1) * window)
        scores = dot_nt(wide.astype(bf16), keys[here, :]) * score_scale
        scores = jnp.where(slot_id < length, scores, -1e30)
        fresh = jnp.sum(wide * fresh_key, axis=1, keepdims=True) * score_scale
        top = jnp.maximum(jnp.max(scores, axis=1, keepdims=True), fresh)
        weights = jnp.exp(scores - top)
        weight_new = jnp.exp(fresh - top)
        total = jnp.sum(weights, axis=1, keepdims=True) + weight_new
        mixed = dot_nn(weights.astype(bf16), values[here, :])
        mixed = (mixed + weight_new * v_row.astype(bf16).astype(f32)) / total
        mixed = mixed.astype(bf16).astype(f32)
        for q in range(heads):
            h = q // per_kv
            att_src[b : b + 1, q * HEAD_SIZE : (q + 1) * HEAD_SIZE] = mixed[
                q : q + 1, h * HEAD_SIZE : (h + 1) * HEAD_SIZE
            ]

    for b in range(own - 1):
        with jax.named_scope("attend"):
            attend(b)
    with jax.named_scope("part_wait"):
        await_landed(part_land.at[pl.ds(0, seq_size - 1)], 1)
    plane_sum = part_land[0].astype(f32)
    for s in range(1, seq_size):
        plane_sum = plane_sum + part_land[s].astype(f32)
    plane_src[...] = plane_sum.astype(bf16)
    plane_land[group] = plane_src[...]
    for _, where in column:
        remote(plane_src, plane_land.at[group], 2, where).start()
    with jax.named_scope("attend"):
        attend(own - 1)
    for _, where in plane:
        remote(att_src, att_land.at[place], 3, where).start()
    att_land[place] = att_src[...]

    with jax.named_scope("mlp"):
        finish("m_gate", "m_up", "m_down", "w_attn")
        hidden = (
            silu(dot_nt(normed, held["m_gate"][...])) * dot_nt(normed, held["m_up"][...])
        ).astype(bf16)
        term[...] = dot_nn(hidden, held["m_down"][...])

    finish("w_step", "step_b", "decay", "skip", "state", "w_out")
    rate = jnp.exp(held["decay"][...])

    with jax.named_scope("cross_wait"):
        await_landed(plane_land.at[pl.ds(0, groups - 1)], 2)

    with jax.named_scope("step_size"):
        low = plane_land[0].astype(f32)
        for z in range(1, groups):
            low = low + plane_land[z].astype(f32)
        low_ref[...] = low
        raw = dot_nn(low[:, :rank].astype(bf16), held["w_step"][...]) + held["step_b"][...]
        step_ref[...] = jnp.maximum(raw, 0.0) + jnp.log1p(jnp.exp(-jnp.abs(raw)))

    def advance(i, carry):
        some = pl.ds(pl.multiple_of(i * 8, 8), 8)
        step = step_ref[some, :][:, None, :]
        conv = conv_ref[some, :][:, None, :]
        tail = low_ref[some, :]
        input_map = tail[:, rank : rank + state_size][:, :, None]
        output_map = tail[:, rank + state_size :][:, :, None]
        fresh = jnp.exp(-step * rate[None]) * held["state"][some] + (step * conv) * input_map
        state_out_ref[some] = fresh
        mix_ref[some, :] = jnp.sum(fresh * output_map, axis=1)
        return carry

    with jax.named_scope("advance"):
        lax.fori_loop(0, rows // 8, advance, 0)
        mixed = mix_ref[...] + held["skip"][...] * conv_ref[...]
        ssm_gated = (mixed * gate_ref[...]).astype(bf16)

    with jax.named_scope("att_wait"):
        await_landed(att_land.at[pl.ds(0, seq_size - 1)], 3)

    with jax.named_scope("attn_out"):
        attended = jnp.concatenate([att_land[s] for s in range(seq_size)], axis=0).astype(bf16)
        col_width = held["w_attn"].shape[1]
        cols = pl.ds(pl.multiple_of(place * col_width, col_width), col_width)
        term[:, cols] += dot_nn(attended, held["w_attn"][...])

    chunk = seq_size * width
    order = sorted(range(groups), key=lambda dg: -min(dg, groups - dg))

    def leave(dg, ds):
        where = (group_at(dg), place_at(ds))
        return remote(
            outgoing.at[where[0] * seq_size + where[1]],
            landed.at[me],
            4,
            where,
        )

    with jax.named_scope("ssm_out"):
        for dg in order:
            base = group_at(dg)
            cols = pl.ds(pl.multiple_of(base * chunk, chunk), chunk)
            block = dot_nn(ssm_gated, held["w_out"][:, cols]) + term[:, cols]
            for s in range(seq_size):
                outgoing[base * seq_size + s] = block[:, s * width : (s + 1) * width].astype(bf16)
            for ds in range(seq_size):
                if dg or ds:
                    leave(dg, ds).start()

    landed[me] = outgoing[me]
    with jax.named_scope("sum_wait"):
        await_landed(landed.at[pl.ds(0, devices - 1)], 4)

    with jax.named_scope("final"):
        total = landed[0].astype(f32)
        for d in range(1, devices):
            total = total + landed[d].astype(f32)
        out_ref[...] = (held["hidden"][...].astype(f32) + total).astype(bf16)
    await_sent(gathered.at[pl.ds(0, devices - 1)], 0)
    await_sent(part_land.at[pl.ds(0, seq_size - 1)], 1)
    await_sent(plane_land.at[pl.ds(0, groups - 1)], 2)
    await_sent(att_land.at[pl.ds(0, seq_size - 1)], 3)
    await_sent(landed.at[pl.ds(0, devices - 1)], 4)


def store_kernel(hidden_ref, state_ref, hidden_out, state_out, sem):
    copies = [
        pltpu.make_async_copy(state_ref, state_out, sem.at[0]),
        pltpu.make_async_copy(hidden_ref, hidden_out, sem.at[1]),
    ]
    for copy in copies:
        copy.start()
    for copy in copies:
        copy.wait()


def rotary_tables(count):
    half_dim = HEAD_SIZE // 2
    frequency = rope_base ** (-(np.arange(half_dim, dtype=np.float32) * 2.0) / HEAD_SIZE)
    angles = np.arange(count, dtype=np.float32)[:, None] * frequency.astype(np.float32)
    cosine, sine = np.cos(angles), np.sin(angles)
    return (
        np.concatenate([cosine, cosine], axis=1).astype(np.float32),
        np.concatenate([-sine, sine], axis=1).astype(np.float32),
    )


def per_device(
    groups,
    seq_size,
    hidden_in,
    norm_gain,
    w_ssm_in,
    w_ssm_gate,
    conv_weight,
    conv_bias,
    conv_state,
    w_state_proj,
    w_step,
    step_bias,
    log_decay,
    skip_gain,
    ssm_state,
    w_ssm_out,
    w_query,
    key_projection,
    value_projection,
    w_attn_out,
    w_mlp_gate,
    w_mlp_up,
    w_mlp_down,
    cached_inputs,
    window_lengths,
):
    rows, width = hidden_in.shape
    devices = groups * seq_size
    model = devices * width
    own, window, _ = cached_inputs.shape
    kv_width, q_width = key_projection.shape[1], w_query.shape[1]
    channels = w_ssm_in.shape[1]
    low_width = w_state_proj.shape[1]
    tile = 256 if window % 256 == 0 else window
    cosine, sine = rotary_tables(window + 8)
    operands = dict(
        hidden=hidden_in,
        gain=norm_gain.reshape(1, -1),
        w_in=w_ssm_in,
        w_gate=w_ssm_gate,
        conv_w=conv_weight,
        conv_b=conv_bias.reshape(1, -1),
        conv_s=conv_state.transpose(1, 0, 2),
        w_state=w_state_proj.T,
        w_step=w_step,
        step_b=step_bias.reshape(1, -1),
        decay=log_decay,
        skip=skip_gain.reshape(1, -1),
        state=ssm_state,
        w_out=w_ssm_out,
        w_query=w_query,
        w_key=key_projection,
        w_value=value_projection,
        w_attn=w_attn_out,
        m_gate=w_mlp_gate.T,
        m_up=w_mlp_up.T,
        m_down=w_mlp_down,
        cached=cached_inputs,
        lengths=window_lengths,
        cosine=jnp.asarray(cosine),
        sine=jnp.asarray(sine),
    )
    dma = pltpu.SemaphoreType.DMA
    hbm_spec = pl.BlockSpec(memory_space=pltpu.HBM)
    vmem_spec = pl.BlockSpec(memory_space=pltpu.VMEM)
    own_copies = [
        (pltpu.SMEM if name == "lengths" else pltpu.VMEM)(operands[name].shape, operands[name].dtype)
        for name in OPERANDS
    ]
    hidden_out, state_out = pl.pallas_call(
        functools.partial(step_kernel, groups, seq_size, w_step.shape[0], tile),
        out_shape=(
            jax.ShapeDtypeStruct((rows, width), bf16),
            jax.ShapeDtypeStruct(ssm_state.shape, f32),
        ),
        in_specs=[hbm_spec] * len(OPERANDS),
        out_specs=(vmem_spec, vmem_spec),
        scratch_shapes=own_copies
        + [
            pltpu.VMEM((devices, rows, width), bf16),
            pltpu.VMEM((rows, model), bf16),
            pltpu.VMEM((own * window, kv_width), bf16),
            pltpu.VMEM((own * window, kv_width), bf16),
            pltpu.VMEM((rows, q_width), f32),
            pltpu.VMEM((rows, kv_width), f32),
            pltpu.VMEM((rows, kv_width), f32),
            pltpu.VMEM((rows, low_width), bf16),
            pltpu.VMEM((seq_size, rows, low_width), bf16),
            pltpu.VMEM((rows, low_width), bf16),
            pltpu.VMEM((groups, rows, low_width), bf16),
            pltpu.VMEM((rows, low_width), f32),
            pltpu.VMEM((rows, channels), f32),
            pltpu.VMEM((rows, channels), f32),
            pltpu.VMEM((rows, channels), f32),
            pltpu.VMEM((rows, channels), f32),
            pltpu.VMEM((own, q_width), f32),
            pltpu.VMEM((seq_size, own, q_width), f32),
            pltpu.VMEM((rows, model), f32),
            pltpu.VMEM((devices, rows, width), bf16),
            pltpu.VMEM((devices, rows, width), bf16),
            pltpu.VMEM((2, rows, channels), f32),
            dma((len(OPERANDS),)),
            dma((len(row_spans(own, window, tile)),)),
            dma((10,)),
        ],
        compiler_params=pltpu.CompilerParams(
            collective_id=0, has_side_effects=True, vmem_limit_bytes=VMEM_LIMIT
        ),
    )(*[pltpu.with_memory_space_constraint(operands[name], pltpu.HBM) for name in OPERANDS])
    return pl.pallas_call(
        store_kernel,
        out_shape=(
            jax.ShapeDtypeStruct((rows, width), bf16),
            jax.ShapeDtypeStruct(ssm_state.shape, f32),
        ),
        in_specs=[vmem_spec] * 2,
        out_specs=(hbm_spec, hbm_spec),
        scratch_shapes=[dma((2,))],
        compiler_params=pltpu.CompilerParams(vmem_limit_bytes=1024 * 1024),
    )(hidden_out, state_out)


def solution(mesh):
    placed = (
        P(None, ("grp", "seq")),
        P(),
        P(None, ("grp", "seq")),
        P(None, ("grp", "seq")),
        P(None, ("grp", "seq")),
        P(("grp", "seq")),
        P(None, None, ("grp", "seq")),
        P(("grp", "seq"), None),
        P(None, ("grp", "seq")),
        P(("grp", "seq")),
        P(None, ("grp", "seq")),
        P(("grp", "seq")),
        P(None, None, ("grp", "seq")),
        P(("grp", "seq"), None),
        P(None, "grp"),
        P(None, "grp"),
        P(None, "grp"),
        P("grp", "seq"),
        P(None, ("grp", "seq")),
        P(None, ("grp", "seq")),
        P(("grp", "seq"), None),
        P("seq", None, None),
        P(),
    )
    return jax.shard_map(
        functools.partial(per_device, mesh.shape["grp"], mesh.shape["seq"]),
        mesh=mesh,
        in_specs=placed,
        out_specs=(P(None, ("grp", "seq")), P(None, None, ("grp", "seq"))),
        check_vma=False,
    )
```

```python
import functools

import jax
import jax.numpy as jnp
import numpy as np
from jax import lax
from jax.experimental import pallas as pl
from jax.experimental.pallas import tpu as pltpu
from jax.sharding import PartitionSpec as P

HEAD_SIZE = 128
MESH = pl.DeviceIdType.MESH
VMEM_LIMIT = 48 * 1024 * 1024
LATE = 1
MEET_LAST = 3
AHEAD = 4
PAIR = 2


def GATHER_ORDER(groups):
    return list(range(groups))


epsilon = 1e-05
rope_base = 10000.0

bf16 = jnp.bfloat16
f32 = jnp.float32


def dot_nn(a, b):
    return jnp.dot(a, b, preferred_element_type=f32)


def dot_nt(a, b):
    return lax.dot_general(a, b, (((1,), (1,)), ((), ())), preferred_element_type=f32)


def row_spans(own, window, tile):
    spans = [(b, at, tile) for b in range(own) for at in range(0, window, tile)]
    if tile % 2 == 0:
        b, at, size = spans[0]
        spans[:1] = [(b, at, size // 2), (b, at + size // 2, size // 2)]
    return spans


def silu(v):
    return v / (1.0 + jnp.exp(-v))


def turned(values, cosine, sine):
    return (values * cosine + pltpu.roll(values, HEAD_SIZE // 2, 1) * sine).astype(bf16)


OPERANDS = (
    "hidden",
    "gain",
    "w_in",
    "w_gate",
    "conv_w",
    "conv_b",
    "conv_s",
    "w_state",
    "w_step",
    "step_b",
    "decay",
    "skip",
    "state",
    "w_out",
    "w_query",
    "w_key",
    "w_value",
    "w_attn",
    "m_gate",
    "m_up",
    "m_down",
    "cached",
    "lengths",
    "cosine",
    "sine",
)


def step_kernel(groups, seq_size, rank, tile, *refs):
    count = len(OPERANDS)
    hbm = dict(zip(OPERANDS, refs[:count]))
    out_ref, state_out_ref = refs[count : count + 2]
    held = dict(zip(OPERANDS, refs[count + 2 : 2 * count + 2]))
    (
        gathered,
        normed_ref,
        keys,
        values,
        query_rows,
        key_rows,
        value_rows,
        part_src,
        part_land,
        plane_src,
        plane_land,
        low_ref,
        step_ref,
        conv_ref,
        mix_ref,
        gate_ref,
        att_src,
        att_land,
        term,
        outgoing,
        landed,
        halves_ref,
        in_sem,
        x_sem,
        link_sem,
    ) = refs[2 * count + 2 :]
    devices = groups * seq_size
    group = lax.axis_index("grp")
    place = lax.axis_index("seq")
    me = group * seq_size + place
    rows, width = held["hidden"].shape
    model = devices * width
    own, window, _ = held["cached"].shape
    kv_width = held["w_key"].shape[1]
    q_width = held["w_query"].shape[1]
    kv_here = kv_width // HEAD_SIZE
    heads = q_width // HEAD_SIZE
    per_kv = heads // kv_here
    state_size = held["decay"].shape[0]

    def group_at(dg):
        return lax.rem(group + dg, groups) if dg else group

    def place_at(ds):
        return lax.rem(place + ds, seq_size) if ds else place

    every = [
        (dg * seq_size + ds, (group_at(dg), place_at(ds)))
        for dg in GATHER_ORDER(groups)
        for ds in range(seq_size)
        if dg or ds
    ]
    plane = [(ds, (group, place_at(ds))) for ds in range(1, seq_size)]
    column = [(dg, (group_at(dg), place)) for dg in range(1, groups)]

    def remote(src, dst, pair, where):
        return pltpu.make_async_remote_copy(
            src_ref=src,
            dst_ref=dst,
            send_sem=link_sem.at[2 * pair],
            recv_sem=link_sem.at[2 * pair + 1],
            device_id=where,
            device_id_type=MESH,
        )

    def await_sent(block, pair):
        pltpu.make_async_copy(block, block, link_sem.at[2 * pair]).wait()

    def await_landed(block, pair):
        pltpu.make_async_copy(block, block, link_sem.at[2 * pair + 1]).wait()

    barrier = pltpu.get_barrier_semaphore()
    for _, where in every:
        pl.semaphore_signal(barrier, inc=1, device_id=where, device_id_type=MESH)

    def load(name):
        return pltpu.make_async_copy(
            hbm[name], held[name], in_sem.at[OPERANDS.index(name)]
        )

    spans = row_spans(own, window, tile)

    def load_x(i):
        b, at, size = spans[i]
        part = (b, pl.ds(at, size))
        return pltpu.make_async_copy(
            hbm["cached"].at[part], held["cached"].at[part], x_sem.at[i]
        )

    def start(*names):
        for name in names:
            load(name).start()

    def finish(*names):
        for name in names:
            load(name).wait()

    waiting = [
        [],
        [],
        ["gain", "conv_w", "conv_b", "conv_s", "lengths"],
        ["w_in", "w_state"],
        ["w_query", "w_gate"],
        ["m_gate", "m_up", "w_step", "step_b", "decay", "skip"],
        ["m_down", "state", "w_attn", "w_out"],
    ]
    start("hidden", "w_key")
    load_x(0).start()
    start("w_value", "cosine", "sine")
    load_x(1).start()

    def meet():
        with jax.named_scope("meet"):
            finish("hidden")
            pl.semaphore_wait(barrier, devices - 1)
        for n in range(groups):
            z = jnp.where(2 * group < groups, groups - 1 - n, n)
            for ds in range(seq_size):
                def go():
                    remote(held["hidden"], gathered.at[me], 0, (z, place_at(ds))).start()
                if ds:
                    go()
                else:
                    pl.when(z != group)(go)
        gathered[me] = held["hidden"][...]

    far = group >= groups // 2
    first_chip = jnp.logical_and(group == 0, place < 2)
    middle = jnp.logical_not(jnp.logical_or(far, first_chip))
    pl.when(far)(meet)
    with jax.named_scope("first_wait"):
        finish("w_key")

    ahead = min(AHEAD, len(spans))
    for n in range(2, ahead):
        load_x(n).start()

    def ready(i):
        load_x(i).wait()
        if i == 0:
            finish("w_value", "cosine", "sine")
        if i + ahead < len(spans):
            load_x(i + ahead).start()
        last = len(waiting) if i + 1 == len(spans) else i + 1
        for names in waiting[i:last]:
            start(*names)

    def project(i):
        b, begin, size = spans[i]
        slots = slice(begin, begin + size)
        x = held["cached"][b, slots, :]
        at = slice(b * window + begin, b * window + begin + size)
        k_rows = dot_nn(x, held["w_key"][...])
        cosine, sine = held["cosine"][slots, :], held["sine"][slots, :]
        for h in range(kv_here):
            cols = slice(h * HEAD_SIZE, (h + 1) * HEAD_SIZE)
            keys[at, cols] = turned(k_rows[:, cols], cosine, sine)
        v_rows = dot_nn(x, held["w_value"][...])
        values[at, :] = v_rows.astype(bf16)


    early = max(len(spans) - LATE, 1)
    i = 0
    while i < early:
        some = range(i, min(early, i + (PAIR if i else 1)))
        for n in some:
            ready(n)
        with jax.named_scope("project"):
            for n in some:
                project(n)
        if i == 0:
            pl.when(middle)(meet)
        i = some[-1] + 1
        if some[0] <= MEET_LAST < i or (i == early and MEET_LAST >= i):
            pl.when(first_chip)(meet)

    finish("gain", "conv_w", "conv_b", "conv_s", "w_in", "w_state")
    past = held["conv_b"][...]
    for k in range(held["conv_s"].shape[0]):
        past = past + held["conv_s"][k].astype(f32) * held["conv_w"][k : k + 1, :]
    conv_ref[...] = past

    with jax.named_scope("gather_wait"):
        await_landed(gathered.at[pl.ds(0, devices - 1)], 0)

    with jax.named_scope("norm"):
        total = jnp.zeros((rows, width), f32)
        for d in range(devices):
            block = gathered[d].astype(f32)
            total = total + block * block
        scale = lax.rsqrt(jnp.sum(total, axis=1, keepdims=True) * (1.0 / model) + epsilon)
        for d in range(devices):
            cols = slice(d * width, (d + 1) * width)
            normed_ref[:, cols] = (gathered[d].astype(f32) * scale * held["gain"][:, cols]).astype(bf16)

    with jax.named_scope("ssm_in"):
        normed = normed_ref[...]
        taps = held["conv_w"].shape[0]
        k_half = model // 2
        halves_ref[0] = dot_nn(normed[:, :k_half], held["w_in"][:k_half, :])
        halves_ref[1] = dot_nn(normed[:, k_half:], held["w_in"][k_half:, :])
        ssm_input = (halves_ref[0] + halves_ref[1]).astype(bf16).astype(f32)
        conv_out = silu(conv_ref[...] + held["conv_w"][taps - 1 : taps, :] * ssm_input)
        conv_ref[...] = conv_out
        part_src[...] = dot_nt(conv_out.astype(bf16), held["w_state"][...]).astype(bf16)

    for _, where in plane:
        remote(part_src, part_land.at[place], 1, where).start()
    part_land[place] = part_src[...]

    for i in range(early, len(spans)):
        ready(i)
    finish("w_query", "w_gate", "lengths")
    with jax.named_scope("qkv_gate"):
        for i in range(early, len(spans)):
            project(i)
        query_rows[...] = dot_nn(normed, held["w_query"][...])
        key_rows[...] = dot_nn(normed, held["w_key"][...])
        value_rows[...] = dot_nn(normed, held["w_value"][...])
        gate_ref[...] = silu(dot_nn(normed, held["w_gate"][...]))

    first = place * own
    score_scale = HEAD_SIZE ** (-0.5)
    padded = -(-heads // 8) * 8
    row_id = lax.broadcasted_iota(jnp.int32, (padded, HEAD_SIZE), 0)
    slot_id = lax.broadcasted_iota(jnp.int32, (padded, window), 1)

    def attend(b):
        length = held["lengths"][first + b]
        q_row = query_rows[pl.ds(first + b, 1), :]
        k_row = key_rows[pl.ds(first + b, 1), :]
        v_row = value_rows[pl.ds(first + b, 1), :]
        cosine = held["cosine"][pl.ds(length, 1), :]
        sine = held["sine"][pl.ds(length, 1), :]
        stacked = jnp.zeros((padded, HEAD_SIZE), f32)
        for q in range(heads):
            stacked = jnp.where(row_id == q, q_row[:, q * HEAD_SIZE : (q + 1) * HEAD_SIZE], stacked)
        query = turned(stacked, cosine, sine).astype(f32)
        wide = jnp.concatenate(
            [
                jnp.where((row_id >= h * per_kv) & (row_id < (h + 1) * per_kv), query, 0.0)
                for h in range(kv_here)
            ],
            axis=1,
        )
        fresh_key = jnp.concatenate(
            [
                turned(k_row[:, h * HEAD_SIZE : (h + 1) * HEAD_SIZE], cosine, sine).astype(f32)
                for h in range(kv_here)
            ],
            axis=1,
        )
        here = slice(b * window, (b + 1) * window)
        scores = dot_nt(wide.astype(bf16), keys[here, :]) * score_scale
        scores = jnp.where(slot_id < length, scores, -1e30)
        fresh = jnp.sum(wide * fresh_key, axis=1, keepdims=True) * score_scale
        top = jnp.maximum(jnp.max(scores, axis=1, keepdims=True), fresh)
        weights = jnp.exp(scores - top)
        weight_new = jnp.exp(fresh - top)
        total = jnp.sum(weights, axis=1, keepdims=True) + weight_new
        mixed = dot_nn(weights.astype(bf16), values[here, :])
        mixed = (mixed + weight_new * v_row.astype(bf16).astype(f32)) / total
        mixed = mixed.astype(bf16).astype(f32)
        for q in range(heads):
            h = q // per_kv
            att_src[b : b + 1, q * HEAD_SIZE : (q + 1) * HEAD_SIZE] = mixed[
                q : q + 1, h * HEAD_SIZE : (h + 1) * HEAD_SIZE
            ]

    for b in range(own - 1):
        with jax.named_scope("attend"):
            attend(b)
    with jax.named_scope("part_wait"):
        await_landed(part_land.at[pl.ds(0, seq_size - 1)], 1)
    plane_sum = part_land[0].astype(f32)
    for s in range(1, seq_size):
        plane_sum = plane_sum + part_land[s].astype(f32)
    plane_src[...] = plane_sum.astype(bf16)
    plane_land[group] = plane_src[...]
    for _, where in column:
        remote(plane_src, plane_land.at[group], 2, where).start()
    with jax.named_scope("attend"):
        attend(own - 1)
    for _, where in plane:
        remote(att_src, att_land.at[place], 3, where).start()
    att_land[place] = att_src[...]

    with jax.named_scope("mlp"):
        finish("m_gate", "m_up", "m_down", "w_attn")
        hidden = (
            silu(dot_nt(normed, held["m_gate"][...])) * dot_nt(normed, held["m_up"][...])
        ).astype(bf16)
        term[...] = dot_nn(hidden, held["m_down"][...])

    finish("w_step", "step_b", "decay", "skip", "state", "w_out")
    rate = jnp.exp(held["decay"][...])

    with jax.named_scope("cross_wait"):
        await_landed(plane_land.at[pl.ds(0, groups - 1)], 2)

    with jax.named_scope("step_size"):
        low = plane_land[0].astype(f32)
        for z in range(1, groups):
            low = low + plane_land[z].astype(f32)
        low_ref[...] = low
        raw = dot_nn(low[:, :rank].astype(bf16), held["w_step"][...]) + held["step_b"][...]
        step_ref[...] = jnp.maximum(raw, 0.0) + jnp.log1p(jnp.exp(-jnp.abs(raw)))

    def advance(i, carry):
        some = pl.ds(pl.multiple_of(i * 8, 8), 8)
        step = step_ref[some, :][:, None, :]
        conv = conv_ref[some, :][:, None, :]
        tail = low_ref[some, :]
        input_map = tail[:, rank : rank + state_size][:, :, None]
        output_map = tail[:, rank + state_size :][:, :, None]
        fresh = jnp.exp(-step * rate[None]) * held["state"][some] + (step * conv) * input_map
        state_out_ref[some] = fresh
        mix_ref[some, :] = jnp.sum(fresh * output_map, axis=1)
        return carry

    with jax.named_scope("advance"):
        lax.fori_loop(0, rows // 8, advance, 0)
        mixed = mix_ref[...] + held["skip"][...] * conv_ref[...]
        ssm_gated = (mixed * gate_ref[...]).astype(bf16)

    with jax.named_scope("att_wait"):
        await_landed(att_land.at[pl.ds(0, seq_size - 1)], 3)

    with jax.named_scope("attn_out"):
        attended = jnp.concatenate([att_land[s] for s in range(seq_size)], axis=0).astype(bf16)
        col_width = held["w_attn"].shape[1]
        cols = pl.ds(pl.multiple_of(place * col_width, col_width), col_width)
        term[:, cols] += dot_nn(attended, held["w_attn"][...])

    chunk = seq_size * width
    def leave(z, ds):
        where = (z, place_at(ds))
        remote(
            outgoing.at[where[0] * seq_size + where[1]],
            landed.at[me],
            4,
            where,
        ).start()

    low_half = 2 * group < groups
    ahead_of = list(reversed(range(groups)))
    with jax.named_scope("ssm_out"):
        for dg in ahead_of:
            step_up = jnp.where(low_half, dg, (groups - dg) % groups)
            base = lax.rem(group + step_up, groups)
            cols = pl.ds(pl.multiple_of(base * chunk, chunk), chunk)
            block = dot_nn(ssm_gated, held["w_out"][:, cols]) + term[:, cols]
            for s in range(seq_size):
                outgoing[base * seq_size + s] = block[:, s * width : (s + 1) * width].astype(bf16)
            for ds in range(seq_size):
                if dg or ds:
                    leave(base, ds)
    landed[me] = outgoing[me]
    with jax.named_scope("sum_wait"):
        await_landed(landed.at[pl.ds(0, devices - 1)], 4)

    with jax.named_scope("final"):
        total = landed[0].astype(f32)
        for d in range(1, devices):
            total = total + landed[d].astype(f32)
        out_ref[...] = (held["hidden"][...].astype(f32) + total).astype(bf16)
    await_sent(gathered.at[pl.ds(0, devices - 1)], 0)
    await_sent(part_land.at[pl.ds(0, seq_size - 1)], 1)
    await_sent(plane_land.at[pl.ds(0, groups - 1)], 2)
    await_sent(att_land.at[pl.ds(0, seq_size - 1)], 3)
    await_sent(landed.at[pl.ds(0, devices - 1)], 4)


def store_kernel(hidden_ref, state_ref, hidden_out, state_out, sem):
    copies = [
        pltpu.make_async_copy(state_ref, state_out, sem.at[0]),
        pltpu.make_async_copy(hidden_ref, hidden_out, sem.at[1]),
    ]
    for copy in copies:
        copy.start()
    for copy in copies:
        copy.wait()


def rotary_tables(count):
    half_dim = HEAD_SIZE // 2
    frequency = rope_base ** (-(np.arange(half_dim, dtype=np.float32) * 2.0) / HEAD_SIZE)
    angles = np.arange(count, dtype=np.float32)[:, None] * frequency.astype(np.float32)
    cosine, sine = np.cos(angles), np.sin(angles)
    return (
        np.concatenate([cosine, cosine], axis=1).astype(np.float32),
        np.concatenate([-sine, sine], axis=1).astype(np.float32),
    )


def per_device(
    groups,
    seq_size,
    hidden_in,
    norm_gain,
    w_ssm_in,
    w_ssm_gate,
    conv_weight,
    conv_bias,
    conv_state,
    w_state_proj,
    w_step,
    step_bias,
    log_decay,
    skip_gain,
    ssm_state,
    w_ssm_out,
    w_query,
    key_projection,
    value_projection,
    w_attn_out,
    w_mlp_gate,
    w_mlp_up,
    w_mlp_down,
    cached_inputs,
    window_lengths,
):
    rows, width = hidden_in.shape
    devices = groups * seq_size
    model = devices * width
    own, window, _ = cached_inputs.shape
    kv_width, q_width = key_projection.shape[1], w_query.shape[1]
    channels = w_ssm_in.shape[1]
    low_width = w_state_proj.shape[1]
    tile = 256 if window % 256 == 0 else window
    cosine, sine = rotary_tables(window + 8)
    operands = dict(
        hidden=hidden_in,
        gain=norm_gain.reshape(1, -1),
        w_in=w_ssm_in,
        w_gate=w_ssm_gate,
        conv_w=conv_weight,
        conv_b=conv_bias.reshape(1, -1),
        conv_s=conv_state.transpose(1, 0, 2),
        w_state=w_state_proj.T,
        w_step=w_step,
        step_b=step_bias.reshape(1, -1),
        decay=log_decay,
        skip=skip_gain.reshape(1, -1),
        state=ssm_state,
        w_out=w_ssm_out,
        w_query=w_query,
        w_key=key_projection,
        w_value=value_projection,
        w_attn=w_attn_out,
        m_gate=w_mlp_gate.T,
        m_up=w_mlp_up.T,
        m_down=w_mlp_down,
        cached=cached_inputs,
        lengths=window_lengths,
        cosine=jnp.asarray(cosine),
        sine=jnp.asarray(sine),
    )
    dma = pltpu.SemaphoreType.DMA
    hbm_spec = pl.BlockSpec(memory_space=pltpu.HBM)
    vmem_spec = pl.BlockSpec(memory_space=pltpu.VMEM)
    own_copies = [
        (pltpu.SMEM if name == "lengths" else pltpu.VMEM)(operands[name].shape, operands[name].dtype)
        for name in OPERANDS
    ]
    hidden_out, state_out = pl.pallas_call(
        functools.partial(step_kernel, groups, seq_size, w_step.shape[0], tile),
        out_shape=(
            jax.ShapeDtypeStruct((rows, width), bf16),
            jax.ShapeDtypeStruct(ssm_state.shape, f32),
        ),
        in_specs=[hbm_spec] * len(OPERANDS),
        out_specs=(vmem_spec, vmem_spec),
        scratch_shapes=own_copies
        + [
            pltpu.VMEM((devices, rows, width), bf16),
            pltpu.VMEM((rows, model), bf16),
            pltpu.VMEM((own * window, kv_width), bf16),
            pltpu.VMEM((own * window, kv_width), bf16),
            pltpu.VMEM((rows, q_width), f32),
            pltpu.VMEM((rows, kv_width), f32),
            pltpu.VMEM((rows, kv_width), f32),
            pltpu.VMEM((rows, low_width), bf16),
            pltpu.VMEM((seq_size, rows, low_width), bf16),
            pltpu.VMEM((rows, low_width), bf16),
            pltpu.VMEM((groups, rows, low_width), bf16),
            pltpu.VMEM((rows, low_width), f32),
            pltpu.VMEM((rows, channels), f32),
            pltpu.VMEM((rows, channels), f32),
            pltpu.VMEM((rows, channels), f32),
            pltpu.VMEM((rows, channels), f32),
            pltpu.VMEM((own, q_width), f32),
            pltpu.VMEM((seq_size, own, q_width), f32),
            pltpu.VMEM((rows, model), f32),
            pltpu.VMEM((devices, rows, width), bf16),
            pltpu.VMEM((devices, rows, width), bf16),
            pltpu.VMEM((2, rows, channels), f32),
            dma((len(OPERANDS),)),
            dma((len(row_spans(own, window, tile)),)),
            dma((10,)),
        ],
        compiler_params=pltpu.CompilerParams(
            collective_id=0, has_side_effects=True, vmem_limit_bytes=VMEM_LIMIT
        ),
    )(*[pltpu.with_memory_space_constraint(operands[name], pltpu.HBM) for name in OPERANDS])
    return pl.pallas_call(
        store_kernel,
        out_shape=(
            jax.ShapeDtypeStruct((rows, width), bf16),
            jax.ShapeDtypeStruct(ssm_state.shape, f32),
        ),
        in_specs=[vmem_spec] * 2,
        out_specs=(hbm_spec, hbm_spec),
        scratch_shapes=[dma((2,))],
        compiler_params=pltpu.CompilerParams(vmem_limit_bytes=1024 * 1024),
    )(hidden_out, state_out)


def solution(mesh):
    placed = (
        P(None, ("grp", "seq")),
        P(),
        P(None, ("grp", "seq")),
        P(None, ("grp", "seq")),
        P(None, ("grp", "seq")),
        P(("grp", "seq")),
        P(None, None, ("grp", "seq")),
        P(("grp", "seq"), None),
        P(None, ("grp", "seq")),
        P(("grp", "seq")),
        P(None, ("grp", "seq")),
        P(("grp", "seq")),
        P(None, None, ("grp", "seq")),
        P(("grp", "seq"), None),
        P(None, "grp"),
        P(None, "grp"),
        P(None, "grp"),
        P("grp", "seq"),
        P(None, ("grp", "seq")),
        P(None, ("grp", "seq")),
        P(("grp", "seq"), None),
        P("seq", None, None),
        P(),
    )
    return jax.shard_map(
        functools.partial(per_device, mesh.shape["grp"], mesh.shape["seq"]),
        mesh=mesh,
        in_specs=placed,
        out_specs=(P(None, ("grp", "seq")), P(None, None, ("grp", "seq"))),
        check_vma=False,
    )
```
